32 devices in a mesh: member: 1 (over z), lat: 32 (over y, x, core).
Axes of the slice: x: 4, y: 4, z: 1, core: 2. Of those that a mesh axis runs over, the one named last changes fastest.
The devices are a block of a 4x4x8 slice.
Arguments:
- field_in: float32 [8, 128, 96, 192], P('member', None, 'lat')
- grad_out: float32 [8, 128, 96, 192], P('member', None, 'lat')
- p_fwd: float32 [96, 96, 96], replicated
- p_inv: float32 [96, 96, 96], replicated
- w_mix: float32 [96, 128, 128, 2], replicated
Outputs:
- output 1: float32 [8, 128, 96, 192], P('member', None, 'lat')
- output 2: float32 [96, 128, 128, 2], P('member')
All inputs are finite; a program needn't handle non-finite values.
Results may differ from the reference program's by a relative error of at most 0.00628536.
Values are sent between devices in bfloat16 or wider.
A program may use at most 768 MiB of HBM per device.

```python
import math
import jax
import jax.numpy as jnp
from jax import lax

BATCH = 8
CHANNELS = 128
NLAT = 96

NLON = 2 * NLAT


def setup_inputs(seed: int = 0, part: int = 0) -> dict:
    part_key = jax.random.fold_in(jax.random.key(seed), part)
    key_field, key_grad = jax.random.split(part_key, 2)
    key_fwd, key_inv, key_mix = jax.random.split(jax.random.key(seed + 1), 3)
    field_in = jax.random.normal(key_field, (BATCH, CHANNELS, NLAT, NLON), jnp.float32)
    grad_out = jax.random.normal(key_grad, (BATCH, CHANNELS, NLAT, NLON), jnp.float32)
    wave_num = jnp.arange(NLAT)[:, None, None]
    degree = jnp.arange(NLAT)[None, :, None]
    lower_tri = (degree >= wave_num).astype(jnp.float32)
    fwd_scale = lower_tri / math.sqrt(NLAT)
    inv_scale = lower_tri / jnp.sqrt((NLAT - wave_num).astype(jnp.float32))
    p_fwd = jax.random.normal(key_fwd, (NLAT, NLAT, NLAT), jnp.float32) * fwd_scale
    p_inv = jax.random.normal(key_inv, (NLAT, NLAT, NLAT), jnp.float32) * inv_scale
    w_mix = jax.random.normal(key_mix, (NLAT, CHANNELS, CHANNELS, 2), jnp.float32) / math.sqrt(2 * CHANNELS)
    return {'field_in': field_in, 'grad_out': grad_out, 'p_fwd': p_fwd, 'p_inv': p_inv, 'w_mix': w_mix}


def to_bf16(values):
    return values.astype(jnp.bfloat16).astype(jnp.float32)


def gelu_grad(values):
    cumulative = 0.5 * (1.0 + lax.erf(values * math.sqrt(0.5)))
    density = jnp.exp(-0.5 * values * values) / math.sqrt(2.0 * math.pi)
    return cumulative + values * density


def mix_matrix(w_mix):
    w_real = w_mix[..., 0]
    w_imag = w_mix[..., 1]
    upper_half = jnp.stack([w_real, -w_imag], axis=-1)
    lower_half = jnp.stack([w_imag, w_real], axis=-1)
    return jnp.stack([upper_half, lower_half], axis=2)


def analysis(values, mode_gains):
    spectrum = jnp.fft.rfft(values, axis=-1)[..., :NLAT] * mode_gains
    return jnp.stack([spectrum.real, spectrum.imag], axis=-2)


def synthesis(spec_pair, mode_gains):
    complex_spec = lax.complex(spec_pair[..., 0, :], spec_pair[..., 1, :]) * mode_gains
    padded = jnp.pad(complex_spec, [(0, 0)] * (complex_spec.ndim - 1) + [(0, NLON // 2 + 1 - NLAT)])
    return jnp.fft.irfft(padded, n=NLON, axis=-1)


def reference(field_in, grad_out, p_fwd, p_inv, w_mix):
    root_lon = math.sqrt(NLON)
    is_mean = jnp.arange(NLAT) == 0
    pw_half = to_bf16(p_fwd)
    pi_half = to_bf16(p_inv)
    w_big = to_bf16(mix_matrix(w_mix))
    four_lat = to_bf16(analysis(field_in, 1.0 / root_lon))
    coeffs = to_bf16(jnp.einsum('mlt,bctrm->bclrm', pw_half, four_lat))
    mixed_coef = to_bf16(jnp.einsum('losir,bilrm->bolsm', w_big, coeffs))
    back_lat = to_bf16(jnp.einsum('mlt,bclrm->bctrm', pi_half, mixed_coef))
    hidden = synthesis(back_lat, root_lon)
    grad_hidden = grad_out * gelu_grad(hidden)
    grad_back = to_bf16(analysis(grad_hidden, jnp.where(is_mean, 1.0, 2.0) / root_lon))
    grad_mixed = to_bf16(jnp.einsum('mlt,bctrm->bclrm', pi_half, grad_back))
    grad_big = jnp.einsum('bolsm,bilrm->losir', grad_mixed, coeffs)
    grad_coef = to_bf16(jnp.einsum('losir,bolsm->bilrm', w_big, grad_mixed))
    grad_four = to_bf16(jnp.einsum('mlt,bclrm->bctrm', pw_half, grad_coef))
    grad_field = grad_out + synthesis(grad_four, jnp.where(is_mean, 1.0, 0.5) * root_lon)
    grad_wmix = jnp.stack([grad_big[:, :, 0, :, 0] + grad_big[:, :, 1, :, 1], grad_big[:, :, 1, :, 0] - grad_big[:, :, 0, :, 1]], axis=-1)
    return grad_field, grad_wmix
```

```python
import functools
import math
import numpy as np
import jax
import jax.numpy as jnp
from jax import lax
from jax.experimental import pallas as pl
from jax.experimental.pallas import tpu as pltpu
from jax.sharding import PartitionSpec as P

MESH = pl.DeviceIdType.MESH
F32, BF16 = jnp.float32, jnp.bfloat16
VMEM = pltpu.VMEM


class Dims:
    def __init__(self, n, batch, chan, rows, lon):
        self.n = n
        self.side = math.isqrt(n // 2)
        self.b, self.c, self.t, self.lon = batch, chan, rows, lon
        self.lat = n * rows
        self.bt = batch * rows
        self.msg = 2 * rows * self.bt
        self.pitch = self.msg + 8
        self.lp = self.lat + 8
        self.ship_off = [batch * j * (j + 1) for j in range(rows + 1)]


def split_const(mat):
    hi = mat.astype(jnp.bfloat16)
    lo = (mat - hi.astype(np.float64)).astype(jnp.bfloat16)
    return hi, lo


def dft_constants(d):
    m = np.arange(d.lat)
    ang = 2.0 * np.pi * np.outer(m, np.arange(d.lon)) / d.lon
    scale = 1.0 / math.sqrt(d.lon)
    ana = scale * np.concatenate([np.cos(ang), -np.sin(ang)])
    gain = np.where(m == 0, 1.0, 2.0)[:, None]
    ana2 = scale * np.concatenate([np.cos(ang) * gain, -np.sin(ang) * gain])
    syn = ana2.T
    syn2 = ana.T
    return [split_const(a) for a in (ana, ana2, syn, syn2)]


def perm_constant(d):
    t = np.arange(d.lat)
    tau = (t % d.t) * d.n + t // d.t
    mat = np.zeros((d.lat, d.lat))
    mat[t, tau] = 1.0
    return mat.astype(jnp.bfloat16)


def mm(a, b):
    return jnp.dot(a, b, preferred_element_type=F32)


def mm_nt(a, b):
    return lax.dot_general(a, b, (((1,), (1,)), ((), ())), preferred_element_type=F32)


def mm_tn(a, b):
    return lax.dot_general(a, b, (((0,), (0,)), ((), ())), preferred_element_type=F32)


def rnd(x):
    return x.astype(BF16).astype(F32)


def target(d, me, k):
    s = d.side
    y, x, h = me // (2 * s), lax.rem(me // 2, s), lax.rem(me, 2)
    dy, dx, dh = k // (2 * s), lax.rem(k // 2, s), lax.rem(k, 2)
    to = lax.rem(y + dy, s) * (2 * s) + lax.rem(x + dx, s) * 2 + lax.rem(h + dh, 2)
    fro = lax.rem(y - dy + s, s) * (2 * s) + lax.rem(x - dx + s, s) * 2 + lax.rem(h + dh, 2)
    return to, fro


def barrier(d, me):
    sem = pltpu.get_barrier_semaphore()

    def body(k, _):
        pl.semaphore_signal(sem, inc=1, device_id={"lat": lax.rem(me + k, d.n)}, device_id_type=MESH)
        return 0
    lax.fori_loop(1, d.n, body, 0)
    pl.semaphore_wait(sem, d.n - 1)


def send_copy(d, me, k, send, recv, ssem, rsem):
    to, _ = target(d, me, k)
    return pltpu.make_async_remote_copy(
        src_ref=send.at[to], dst_ref=recv.at[me], send_sem=ssem.at[k], recv_sem=rsem.at[k],
        device_id={"lat": to}, device_id_type=MESH)


def exchange(d, me, send, recv, ssem, rsem):
    recv[me] = send[me]

    def start(k, _):
        send_copy(d, me, k, send, recv, ssem, rsem).start()
        return 0

    def wait(k, _):
        send_copy(d, me, k, send, recv, ssem, rsem).wait()
        return 0
    lax.fori_loop(1, d.n, start, 0)
    lax.fori_loop(1, d.n, wait, 0)


def to_messages(d, stage, send):
    def body(s, _):
        send[s] = stage[pl.ds(pl.multiple_of(s * d.pitch, 8), d.msg), :].astype(BF16)
        return 0
    lax.fori_loop(0, d.n, body, 0)


def from_messages(d, recv, stage):
    def body(s, _):
        stage[pl.ds(pl.multiple_of(s * d.pitch, 8), d.msg), :] = recv[s].astype(F32)
        return 0
    lax.fori_loop(0, d.n, body, 0)


def ring_rows(d, start):
    return pl.ds(start, d.n, stride=d.pitch)


def put_modes(d, stage, y, bt, lanes):
    for rk in range(2 * d.t):
        stage[ring_rows(d, rk * d.bt + bt), :] = y[rk * d.n:(rk + 1) * d.n, lanes]


def get_modes(d, stage, bt):
    return jnp.concatenate([stage[ring_rows(d, rk * d.bt + bt), :] for rk in range(2 * d.t)], axis=0)


def analyse(x, hi, lo):
    xh = x.astype(BF16)
    xl = (x - xh.astype(F32)).astype(BF16)
    return mm(hi[...], xh) + mm(lo[...], xh) + mm(hi[...], xl)


def pairs(d, body):
    def step(p, _):
        body(2 * p)
        return 0
    lax.fori_loop(0, d.bt // 2, step, 0)


def lane_halves(d):
    return slice(0, d.c), slice(d.c, 2 * d.c)


def permuted(d, perm, p, out, outt):
    for k in range(d.t):
        pk = p[k].astype(BF16)
        if out is not None:
            out[k] = mm(pk, perm[...]).astype(BF16)
        if outt is not None:
            outt[k] = mm_tn(perm[...], pk.T).astype(BF16)


def spec_rows(d, r, k, b):
    return pl.ds(pl.multiple_of(((r * d.t + k) * d.b + b) * d.lp, 8), d.lat)


def to_spectral(d, stage, spec, p):
    for k in range(d.t):
        def body(b, _):
            x = jnp.concatenate([jnp.concatenate(
                [stage[ring_rows(d, (r * d.t + k) * d.bt + b * d.t + t), :] for t in range(d.t)], axis=0)
                for r in range(2)], axis=1)
            y = rnd(mm(p[k], x.astype(BF16)))
            for r, half in enumerate(lane_halves(d)):
                spec[spec_rows(d, r, k, b), :] = y[:, half]
            return 0
        lax.fori_loop(0, d.b, body, 0)


def from_spectral(d, spec, stage, pt):
    for k in range(d.t):
        def body(b, _):
            x = jnp.concatenate([spec[spec_rows(d, r, k, b), :] for r in range(2)], axis=1).astype(BF16)
            y = mm(pt[k], x)
            for r, half in enumerate(lane_halves(d)):
                for t in range(d.t):
                    stage[ring_rows(d, (r * d.t + k) * d.bt + b * d.t + t), :] = y[t * d.n:(t + 1) * d.n, half]
            return 0
        lax.fori_loop(0, d.b, body, 0)


def mix(d, spec, w, ship, forward):
    half = d.t * d.b * d.lp
    for j in range(d.t):
        rows = d.b * (j + 1)

        def body(ll, _):
            l = d.n * j + ll
            at = [pl.ds(r * half + l, rows, stride=d.lp) for r in range(2)]
            x = jnp.concatenate([spec[at[0], :], spec[at[1], :]], axis=0).astype(BF16)
            ship[ll, d.ship_off[j]:d.ship_off[j + 1], :] = x
            wp = [w[pl.ds(l * 2 * d.c + r, d.c, stride=2), :].astype(BF16) for r in range(2)]
            if forward:
                y = mm_nt(x, jnp.concatenate(wp, axis=0))
                re = y[:rows, :d.c] - y[rows:, d.c:]
                im = y[rows:, :d.c] + y[:rows, d.c:]
            else:
                y = mm(x, jnp.concatenate(wp, axis=1))
                re = y[:rows, :d.c] + y[rows:, d.c:]
                im = y[rows:, :d.c] - y[:rows, d.c:]
            spec[at[0], :] = rnd(re)
            spec[at[1], :] = rnd(im)
            return 0
        lax.fori_loop(0, d.n, body, 0)


def gelu_grad(values):
    cumulative = 0.5 * (1.0 + lax.erf(values * math.sqrt(0.5)))
    density = jnp.exp(-0.5 * values * values) * (1.0 / math.sqrt(2.0 * math.pi))
    return cumulative + values * density


def analysis_kernel(d, f, hi, lo, recv, stage, send, ssem, rsem):
    me = lax.axis_index("lat")
    barrier(d, me)

    def body(bt):
        y = analyse(jnp.concatenate([f[bt], f[bt + 1]], axis=1), hi, lo)
        for u, half in enumerate(lane_halves(d)):
            put_modes(d, stage, y, bt + u, half)
    pairs(d, body)
    to_messages(d, stage, send)
    exchange(d, me, send, recv, ssem, rsem)


def spectral_kernel(d, forward, got, pin, pout, perm, w, recv, ship_recv, stage, spec, send, ship, p, pt, ssem, rsem, ssem2, rsem2):
    me = lax.axis_index("lat")
    barrier(d, me)
    permuted(d, perm, pin, p, None)
    permuted(d, perm, pout, None, pt)
    from_messages(d, got, stage)
    to_spectral(d, stage, spec, p)
    mix(d, spec, w, ship, forward)
    from_spectral(d, spec, stage, pt)
    to_messages(d, stage, send)
    exchange(d, me, send, recv, ssem, rsem)
    exchange(d, me, ship, ship_recv, ssem2, rsem2)


def grid_kernel(d, got, dg, shi, slo, ahi, alo, recv, stage, send, ssem, rsem):
    me = lax.axis_index("lat")
    barrier(d, me)
    from_messages(d, got, stage)

    def body(bt):
        g = jnp.concatenate([get_modes(d, stage, bt), get_modes(d, stage, bt + 1)], axis=1).astype(BF16)
        h = mm(shi[...], g) + mm(slo[...], g)
        u = jnp.concatenate([dg[bt], dg[bt + 1]], axis=1) * gelu_grad(h)
        y = analyse(u, ahi, alo)
        for i, half in enumerate(lane_halves(d)):
            put_modes(d, stage, y, bt + i, half)
    pairs(d, body)
    to_messages(d, stage, send)
    exchange(d, me, send, recv, ssem, rsem)


def weight_kernel(d, a, dq, out):
    for j in range(d.t):
        rows = d.b * (j + 1)
        at = slice(d.ship_off[j], d.ship_off[j + 1])
        aj = a[:, at, :]
        swapped = jnp.concatenate([-aj[:, rows:], aj[:, :rows]], axis=1)
        both = jnp.concatenate([aj, swapped], axis=2).reshape(d.n * 2 * rows, 2 * d.c)
        y = mm_tn(dq[:, at, :].reshape(d.n * 2 * rows, d.c), both)
        for r, half in enumerate(lane_halves(d)):
            out[pl.ds(j * 2 * d.c + r, d.c, stride=2), :] = y[:, half]


def final_kernel(d, got, dg, shi, slo, out, stage):
    from_messages(d, got, stage)

    def body(bt):
        g = jnp.concatenate([get_modes(d, stage, bt), get_modes(d, stage, bt + 1)], axis=1).astype(BF16)
        y = mm(shi[...], g) + mm(slo[...], g)
        for i, half in enumerate(lane_halves(d)):
            out[bt + i] = dg[bt + i] + y[:, half]
    pairs(d, body)


def call(name, kernel, outs, scratch, args, cid=None):
    single = not isinstance(outs, (list, tuple))
    spec = pl.BlockSpec(memory_space=VMEM)
    params = dict(vmem_limit_bytes=60 * 1024 * 1024)
    if cid is not None:
        params.update(collective_id=cid, has_side_effects=True)
    return pl.pallas_call(
        kernel, name=name, out_shape=outs, in_specs=[spec] * len(args),
        out_specs=spec if single else [spec] * len(outs), scratch_shapes=scratch,
        compiler_params=pltpu.CompilerParams(**params))(*args)


def solution(mesh):
    n = mesh.shape['lat']
    field_spec = P('member', None, 'lat', None)

    def local_step(field_loc, grad_loc, p_fwd, p_inv, w_mix):
        batch, chan, rows, lon = field_loc.shape
        d = Dims(n, batch, chan, rows, lon)
        (ah, al), (bh, bl), (sh, sl), (zh, zl) = dft_constants(d)
        perm = perm_constant(d)
        me = lax.axis_index('lat')
        f = field_loc.transpose(0, 2, 3, 1).reshape(d.bt, lon, chan)
        dg = grad_loc.transpose(0, 2, 3, 1).reshape(d.bt, lon, chan)
        w = w_mix.transpose(0, 1, 3, 2).reshape(-1, chan)
        own = lambda p: lax.dynamic_index_in_dim(p.reshape(d.t, n, d.lat, d.lat), me, 1, False)
        pw, pi = own(p_fwd), own(p_inv)

        msgs = jax.ShapeDtypeStruct((n, d.msg, chan), BF16)
        ships = jax.ShapeDtypeStruct((n, d.ship_off[-1], chan), BF16)
        stage = VMEM((n * d.pitch, chan), F32)
        spec = VMEM((2 * d.t * d.b * d.lp, chan), F32)
        mat = VMEM((d.t, d.lat, d.lat), BF16)
        dma = pltpu.SemaphoreType.DMA((n,))
        sems = [dma, dma]
        buf = lambda s: VMEM(s.shape, s.dtype)

        r1 = call("ana", functools.partial(analysis_kernel, d), msgs, [stage, buf(msgs)] + sems, [f, ah, al], 0)
        spec_scratch = [stage, spec, buf(msgs), buf(ships), mat, mat] + sems + sems
        r2, ship_a = call("fwd", functools.partial(spectral_kernel, d, True), [msgs, ships], spec_scratch, [r1, pw, pi, perm, w], 1)
        r3 = call("grid", functools.partial(grid_kernel, d), msgs, [stage, buf(msgs)] + sems, [r2, dg, sh, sl, bh, bl], 2)
        r4, ship_q = call("bwd", functools.partial(spectral_kernel, d, False), [msgs, ships], spec_scratch, [r3, pi, pw, perm, w], 3)
        dw = call("wgt", functools.partial(weight_kernel, d), jax.ShapeDtypeStruct((d.t * 2 * chan, chan), F32), [], [ship_a, ship_q])
        gathered = lax.all_gather(dw.reshape(d.t, 1, 2 * chan, chan), 'lat', axis=1, tiled=True)
        df = call("fin", functools.partial(final_kernel, d), jax.ShapeDtypeStruct((d.bt, lon, chan), F32), [stage], [r4, dg, zh, zl])
        grad_field = df.reshape(batch, rows, lon, chan).transpose(0, 3, 1, 2)
        grad_wmix = gathered.reshape(d.lat, chan, 2, chan).transpose(0, 1, 3, 2)
        return grad_field, grad_wmix

    return jax.shard_map(local_step, mesh=mesh, in_specs=(field_spec, field_spec, P(), P(), P()), out_specs=(field_spec, P('member', None, None, None)), check_vma=False)
```

```python
import functools
import math
import numpy as np
import jax
import jax.numpy as jnp
from jax import lax
from jax.experimental import pallas as pl
from jax.experimental.pallas import tpu as pltpu
from jax.sharding import PartitionSpec as P

MESH = pl.DeviceIdType.MESH
F32, BF16 = jnp.float32, jnp.bfloat16
VMEM = pltpu.VMEM


class Dims:
    def __init__(self, n, batch, chan, rows, lon):
        self.n = n
        self.side = math.isqrt(n // 2)
        self.b, self.c, self.t, self.lon = batch, chan, rows, lon
        self.lat = n * rows
        self.bt = batch * rows
        self.msg = 2 * rows * self.bt
        self.pitch = self.msg + 8
        self.lp = self.lat + 8
        self.ship_off = [batch * j * (j + 1) for j in range(rows + 1)]


def split_const(mat):
    hi = mat.astype(jnp.bfloat16)
    lo = (mat - hi.astype(np.float64)).astype(jnp.bfloat16)
    return hi, lo


def dft_constants(d):
    m = np.arange(d.lat)
    ang = 2.0 * np.pi * np.outer(m, np.arange(d.lon)) / d.lon
    scale = 1.0 / math.sqrt(d.lon)
    ana = scale * np.concatenate([np.cos(ang), -np.sin(ang)])
    gain = np.where(m == 0, 1.0, 2.0)[:, None]
    ana2 = scale * np.concatenate([np.cos(ang) * gain, -np.sin(ang) * gain])
    syn = ana2.T
    syn2 = ana.T
    return [split_const(a) for a in (ana, ana2, syn, syn2)]


def perm_constant(d):
    t = np.arange(d.lat)
    tau = (t % d.t) * d.n + t // d.t
    mat = np.zeros((d.lat, d.lat))
    mat[t, tau] = 1.0
    return mat.astype(jnp.bfloat16)


def mm(a, b):
    return jnp.dot(a, b, preferred_element_type=F32)


def mm_nt(a, b):
    return lax.dot_general(a, b, (((1,), (1,)), ((), ())), preferred_element_type=F32)


def mm_tn(a, b):
    return lax.dot_general(a, b, (((0,), (0,)), ((), ())), preferred_element_type=F32)


def rnd(x):
    return x.astype(BF16).astype(F32)


def place(d, me):
    return me // (2 * d.side), lax.rem(me // 2, d.side), lax.rem(me, 2)


def shifted(d, me, dy, dx, dh):
    y, x, h = place(d, me)
    s = d.side
    return (lax.rem(y + dy + 2 * s, s) * s + lax.rem(x + dx + 2 * s, s)) * 2 + lax.rem(h + dh, 2)


def remote(src, dst, ssem, rsem, to):
    return pltpu.make_async_remote_copy(src_ref=src, dst_ref=dst, send_sem=ssem, recv_sem=rsem,
                                        device_id={"lat": to}, device_id_type=MESH)


def barrier(d, me):
    sem = pltpu.get_barrier_semaphore()

    def body(k, _):
        pl.semaphore_signal(sem, inc=1, device_id={"lat": lax.rem(me + k, d.n)}, device_id_type=MESH)
        return 0
    lax.fori_loop(1, d.n, body, 0)
    pl.semaphore_wait(sem, d.n - 1)


class Exchange:
    def __init__(self, d, me, send, recv, hold, ssem, rsem, hsem, hrecv, fsem):
        self.d, self.me, self.send, self.recv, self.hold = d, me, send, recv, hold
        self.ssem, self.rsem, self.hsem, self.hrecv, self.fsem = ssem, rsem, hsem, hrecv, fsem
        half = d.side // 2
        self.relayed = [(dy, dx) for dy in range(d.side) for dx in range(d.side) if half in (dy, dx)]
        self.half = half

    def key(self, dy, dx, dh):
        return (dy * self.d.side + dx) * 2 + dh

    def direct(self, dy, dx, dh):
        k = self.key(dy, dx, dh)
        to = shifted(self.d, self.me, dy, dx, dh)
        return to, remote(self.send.at[to], self.recv.at[self.me], self.ssem.at[k], self.rsem.at[k], to)

    def hop(self, dy, dx):
        return -int(dy == self.half), -int(dx == self.half)

    def relay_out(self, i):
        dy, dx = self.relayed[i]
        ry, rx = self.hop(dy, dx)
        to = shifted(self.d, self.me, dy, dx, 1)
        via = shifted(self.d, self.me, ry, rx, 0)
        return to, remote(self.send.at[to], self.hold.at[i], self.hsem.at[i], self.hrecv.at[i], via)

    def relay_on(self, i):
        dy, dx = self.relayed[i]
        ry, rx = self.hop(dy, dx)
        origin = shifted(self.d, self.me, -ry, -rx, 0)
        to = shifted(self.d, origin, dy, dx, 1)
        return remote(self.hold.at[i], self.recv.at[origin], self.fsem.at[i], self.rsem.at[self.key(dy, dx, 1)], to)

    def directs(self, body):
        s, half = self.d.side, self.half

        def even(i, _):
            body((i + 1) // s, lax.rem(i + 1, s), 0)
            return 0
        lax.fori_loop(0, s * s - 1, even, 0)

        def odd(i, _):
            a, b = i // (s - 1), lax.rem(i, s - 1)
            body(a + a // half, b + b // half, 1)
            return 0
        lax.fori_loop(0, (s - 1) * (s - 1), odd, 0)

    def dispatch(self, fill):
        for i in range(len(self.relayed)):
            to, copy = self.relay_out(i)
            fill(to)
            copy.start()

        def body(dy, dx, dh):
            to, copy = self.direct(dy, dx, dh)
            fill(to)
            copy.start()
        self.directs(body)
        fill(self.me)

    def forward(self):
        for i in range(len(self.relayed)):
            self.relay_out(i)[1].wait_recv()
            self.relay_on(i).start()

    def collect(self, take):
        take(self.me, self.send)

        def body(dy, dx, dh):
            self.direct(dy, dx, dh)[1].wait_recv()
            take(shifted(self.d, self.me, -dy, -dx, dh), self.recv)
        self.directs(body)
        for dy, dx in self.relayed:
            self.direct(dy, dx, 1)[1].wait_recv()
            take(shifted(self.d, self.me, -dy, -dx, 1), self.recv)

    def drain(self):
        self.directs(lambda dy, dx, dh: self.direct(dy, dx, dh)[1].wait_send())
        for i in range(len(self.relayed)):
            self.relay_out(i)[1].wait_send()
            self.relay_on(i).wait_send()


def message_rows(d, s):
    return pl.ds(pl.multiple_of(s * d.pitch, 8), d.msg)


def ring_rows(d, start):
    return pl.ds(start, d.n, stride=d.pitch)


def put_modes(d, stage, y, bt, lanes):
    for rk in range(2 * d.t):
        stage[ring_rows(d, rk * d.bt + bt), :] = y[rk * d.n:(rk + 1) * d.n, lanes]


def get_modes(d, stage, bt):
    return jnp.concatenate([stage[ring_rows(d, rk * d.bt + bt), :] for rk in range(2 * d.t)], axis=0)


def analyse(x, hi, lo):
    xh = x.astype(BF16)
    xl = (x - xh.astype(F32)).astype(BF16)
    return mm(hi[...], xh) + mm(lo[...], xh) + mm(hi[...], xl)


def loop(count, body, unroll=1):
    def step(i, _):
        body(i)
        return 0
    lax.fori_loop(0, count, step, 0, unroll=unroll)


def lane_halves(d):
    return slice(0, d.c), slice(d.c, 2 * d.c)


def permuted(d, perm, p, out, outt):
    for k in range(d.t):
        pk = p[k].astype(BF16)
        out[k] = mm(pk, perm[...]).astype(BF16)
        outt[k] = mm_tn(perm[...], pk.T).astype(BF16)


def to_spectral(d, stage, spec, p):
    for k in range(d.t):
        low = d.n * k

        def body(b):
            x = jnp.concatenate([jnp.concatenate(
                [stage[ring_rows(d, (r * d.t + k) * d.bt + b * d.t + t), :] for t in range(d.t)], axis=0)
                for r in range(2)], axis=1)
            y = rnd(mm(p[k, low:, :], x.astype(BF16)))
            for r, half in enumerate(lane_halves(d)):
                at = pl.multiple_of(((r * d.t + k) * d.b + b) * d.lp + low, 8)
                spec[pl.ds(at, d.lat - low), :] = y[:, half]
        loop(d.b, body, 4)


def from_spectral(d, spec, stage, pt):
    for k in range(d.t):
        low = d.n * k

        def body(b):
            at = [pl.multiple_of(((r * d.t + k) * d.b + b) * d.lp + low, 8) for r in range(2)]
            x = jnp.concatenate([spec[pl.ds(a, d.lat - low), :] for a in at], axis=1).astype(BF16)
            y = mm(pt[k][:, low:], x)
            for r, half in enumerate(lane_halves(d)):
                for t in range(d.t):
                    stage[ring_rows(d, (r * d.t + k) * d.bt + b * d.t + t), :] = y[t * d.n:(t + 1) * d.n, half]
        loop(d.b, body, 4)


def mix(d, spec, out, w, ship, forward):
    half = d.t * d.b * d.lp
    for j in range(d.t):
        rows = d.b * (j + 1)

        def body(ll):
            l = d.n * j + ll
            at = [pl.ds(r * half + l, rows, stride=d.lp) for r in range(2)]
            x = jnp.concatenate([spec[at[0], :], spec[at[1], :]], axis=0).astype(BF16)
            ship[ll, d.ship_off[j]:d.ship_off[j + 1], :] = x
            wp = [w[pl.ds(l * 2 * d.c + r, d.c, stride=2), :].astype(BF16) for r in range(2)]
            if forward:
                y = mm_nt(x, jnp.concatenate(wp, axis=0))
                re = y[:rows, :d.c] - y[rows:, d.c:]
                im = y[rows:, :d.c] + y[:rows, d.c:]
            else:
                y = mm(x, jnp.concatenate(wp, axis=1))
                re = y[:rows, :d.c] + y[rows:, d.c:]
                im = y[rows:, :d.c] - y[:rows, d.c:]
            out[at[0], :] = rnd(re)
            out[at[1], :] = rnd(im)
        loop(d.n, body, 4)


def gelu_grad(values):
    cumulative = 0.5 * (1.0 + lax.erf(values * math.sqrt(0.5)))
    density = jnp.exp(-0.5 * values * values) * (1.0 / math.sqrt(2.0 * math.pi))
    return cumulative + values * density


def weights(d, a, dq, out, me):
    for j in range(d.t):
        rows = d.b * (j + 1)
        at = slice(d.ship_off[j], d.ship_off[j + 1])
        aj = a[:, at, :]
        swapped = jnp.concatenate([-aj[:, rows:], aj[:, :rows]], axis=1)
        both = jnp.concatenate([aj, swapped], axis=2).reshape(d.n * 2 * rows, 2 * d.c)
        y = mm_tn(dq[:, at, :].reshape(d.n * 2 * rows, d.c), both)
        for r, half in enumerate(lane_halves(d)):
            out[j, me, pl.ds(r, d.c, stride=2), :] = y[:, half]


class Gather:
    def __init__(self, d, me, full, s1, r1, s2, r2, sp, rp):
        self.d, self.me, self.full = d, me, full
        self.s1, self.r1, self.s2, self.r2, self.sp, self.rp = s1, r1, s2, r2, sp, rp
        self.h = lax.rem(me, 2)
        self.half = full.shape[2] // 2
        self.sent = []

    def near(self, dev, first, second):
        h = self.h
        return shifted(self.d, dev, first * h + second * (1 - h), first * (1 - h) + second * h, 0)

    def piece(self, block, part):
        if part is None:
            return self.full.at[:, block]
        return self.full.at[:, block, self.half * part:self.half * (part + 1), :]

    def copy(self, block, part, ssem, rsem, to):
        ref = self.piece(block, part)
        return remote(ref, ref, ssem, rsem, to)

    def start(self, *args):
        c = self.copy(*args)
        c.start()
        self.sent.append(c)

    def arrive(self, block, part, rsem):
        self.copy(block, part, self.sp.at[0], rsem, self.partner).wait_recv()

    def run(self, between):
        me, near, s1, r1, s2, r2, sp, rp = self.me, self.near, self.s1, self.r1, self.s2, self.r2, self.sp, self.rp
        p1, m1, o1 = near(me, 1, 0), near(me, -1, 0), near(me, 2, 0)
        p2, m2 = near(me, 0, 1), near(me, 0, -1)
        self.partner = shifted(self.d, me, 0, 0, 1)
        group = [me, m1, p1, o1]

        def second(q):
            self.start(group[q], None, s2.at[q, 0], r2.at[q, 0], p2)
            self.start(group[q], None, s2.at[q, 1], r2.at[q, 1], m2)
            self.start(group[q], None, sp.at[q], rp.at[q], self.partner)

        def relay(q):
            for i, (off, to) in enumerate(((-1, p2), (1, m2))):
                block = near(group[q], 0, off)
                self.arrive(block, None, r2.at[q, i])
                self.start(block, i, s2.at[q, 2 + i], r2.at[q, 2 + i], to)
                self.start(block, None, sp.at[4 + 2 * q + i], rp.at[4 + 2 * q + i], self.partner)

        self.start(me, None, s1.at[0], r1.at[0], p1)
        self.start(me, None, s1.at[1], r1.at[1], m1)
        second(0)
        between()
        self.arrive(m1, None, r1.at[0])
        self.start(m1, 0, s1.at[2], r1.at[2], p1)
        second(1)
        self.arrive(p1, None, r1.at[1])
        self.start(p1, 1, s1.at[3], r1.at[3], m1)
        second(2)
        relay(0)
        self.arrive(o1, 0, r1.at[2])
        self.arrive(o1, 1, r1.at[3])
        second(3)
        for q in (1, 2, 3):
            relay(q)
        for q in range(4):
            block = near(group[q], 0, 2)
            for i in range(2):
                self.arrive(block, i, r2.at[q, 2 + i])
            self.start(block, None, sp.at[12 + q], rp.at[12 + q], self.partner)
        for i in range(16):
            self.arrive(self.partner, None, rp.at[i])
        for c in self.sent:
            c.wait_send()


def main_kernel(d, f_h, dg_h, w_h, pf_h, pi_h, perm, ah, al, bh, bl, sh, sl, recv4, full,
                f, dg, w, pf, pi, pw, pwt, pv, pvt, stage, stage2, spec, spec2, send, recv, hold, ship, shipr, shold,
                isem, ssem, rsem, hsem, hrecv, fsem, s1, r1, s2, r2, sp, rp):
    me = lax.axis_index("lat")
    step = 6
    loads = [pltpu.make_async_copy(f_h.at[i:i + step], f.at[i:i + step], isem.at[i // step]) for i in range(0, d.bt, step)]
    nf = len(loads)
    rest = []
    for k in range(d.t):
        rest.append(pltpu.make_async_copy(pf_h.at[me + k * d.n], pf.at[k], isem.at[nf + 2 * k]))
        rest.append(pltpu.make_async_copy(pi_h.at[me + k * d.n], pi.at[k], isem.at[nf + 2 * k + 1]))
    wload = pltpu.make_async_copy(w_h, w, isem.at[nf + 6])
    gload = pltpu.make_async_copy(dg_h, dg, isem.at[nf + 7])
    for c in loads + rest + [wload, gload]:
        c.start()
    barrier(d, me)

    def exchange(e, snd, rcv, hld):
        return Exchange(d, me, snd, rcv, hld, ssem.at[e], rsem.at[e], hsem.at[e], hrecv.at[e], fsem.at[e])

    ex = [exchange(i, send.at[i], recv.at[i] if i < 3 else recv4, hold.at[i]) for i in range(4)]
    ships = [exchange(4 + i, ship.at[i], shipr.at[i], shold.at[i]) for i in range(2)]

    def fill(e, st):
        def go(s):
            send[e, s] = st[message_rows(d, s), :].astype(BF16)
        return go

    def take(st):
        def go(s, ref):
            st[message_rows(d, s), :] = ref[s].astype(F32)
        return go

    none = lambda *a: None

    for c in range(nf):
        loads[c].wait()

        def analysis_step(p):
            bt = c * step + 2 * p
            y = analyse(jnp.concatenate([f[bt], f[bt + 1]], axis=1), ah, al)
            for u, half in enumerate(lane_halves(d)):
                put_modes(d, stage, y, bt + u, half)
        loop(step // 2, analysis_step, 3)
    ex[0].dispatch(fill(0, stage))
    for c in rest:
        c.wait()
    permuted(d, perm, pf, pw, pwt)
    permuted(d, perm, pi, pv, pvt)
    ex[0].forward()
    ex[0].collect(take(stage2))
    to_spectral(d, stage2, spec, pw)
    wload.wait()
    mix(d, spec, spec2, w, ship.at[0], True)
    from_spectral(d, spec2, stage, pvt)
    ex[1].dispatch(fill(1, stage))
    ships[0].dispatch(none)
    gload.wait()
    ex[1].forward()
    ex[1].collect(take(stage2))

    def grid_step(p):
        bt = 2 * p
        g = jnp.concatenate([get_modes(d, stage2, bt), get_modes(d, stage2, bt + 1)], axis=1).astype(BF16)
        h = mm(sh[...], g) + mm(sl[...], g)
        u = jnp.concatenate([dg[bt], dg[bt + 1]], axis=1) * gelu_grad(h)
        y = analyse(u, bh, bl)
        for i, half in enumerate(lane_halves(d)):
            put_modes(d, stage, y, bt + i, half)
    loop(d.bt // 2, grid_step, 2)
    ex[2].dispatch(fill(2, stage))
    ships[0].forward()
    ex[2].forward()
    ex[2].collect(take(stage2))
    to_spectral(d, stage2, spec, pv)
    mix(d, spec, spec2, w, ship.at[1], False)
    ships[1].dispatch(none)
    from_spectral(d, spec2, stage, pwt)
    ex[3].dispatch(fill(3, stage))
    recv4[me] = send[3, me]

    def ship_take(i):
        def go(s, ref):
            @pl.when(s == me)
            def _():
                shipr[i, s] = ship[i, s]
        return go
    ships[0].collect(ship_take(0))
    ships[1].forward()
    ships[1].collect(ship_take(1))
    weights(d, shipr.at[0], shipr.at[1], full, me)
    gather = Gather(d, me, full, s1, r1, s2, r2, sp, rp)
    gather.run(ex[3].forward)
    ex[3].collect(none)
    for e in ex + ships:
        e.drain()


def final_kernel(d, got, dg_h, full, shi, slo, out, dw, dg, stage, sem):
    copy = pltpu.make_async_copy(full, dw, sem.at[0])
    load = pltpu.make_async_copy(dg_h, dg, sem.at[1])
    copy.start()
    load.start()

    def take(s):
        stage[message_rows(d, s), :] = got[s].astype(F32)
    loop(d.n, take, 2)
    load.wait()

    def body(p):
        bt = 2 * p
        g = jnp.concatenate([get_modes(d, stage, bt), get_modes(d, stage, bt + 1)], axis=1).astype(BF16)
        y = mm(shi[...], g) + mm(slo[...], g)
        for i, half in enumerate(lane_halves(d)):
            out[bt + i] = dg[bt + i] + y[:, half]
    loop(d.bt // 2, body, 2)
    copy.wait()


def solution(mesh):
    n = mesh.shape['lat']
    field_spec = P('member', None, 'lat', None)

    def local_step(field_loc, grad_loc, p_fwd, p_inv, w_mix):
        batch, chan, rows, lon = field_loc.shape
        d = Dims(n, batch, chan, rows, lon)
        (ah, al), (bh, bl), (sh, sl), (zh, zl) = dft_constants(d)
        perm = perm_constant(d)
        f = field_loc.transpose(0, 2, 3, 1).reshape(d.bt, lon, chan)
        dg = grad_loc.transpose(0, 2, 3, 1).reshape(d.bt, lon, chan)
        w = w_mix.transpose(0, 1, 3, 2).reshape(-1, chan)

        nr = 2 * d.side - 1
        sl_rows = d.ship_off[-1]
        stage = VMEM((n * d.pitch, chan), F32)
        spec = VMEM((2 * rows * batch * d.lp, chan), F32)
        mat = VMEM((rows, d.lat, d.lat), BF16)
        raw = VMEM((rows, d.lat, d.lat), F32)
        field = VMEM((d.bt, lon, chan), F32)
        dma = lambda *s: pltpu.SemaphoreType.DMA(s)
        vspec = pl.BlockSpec(memory_space=VMEM)
        aspec = pl.BlockSpec(memory_space=pl.ANY)
        recv4, full = pl.pallas_call(
            functools.partial(main_kernel, d), name="main",
            out_shape=[VMEM((n, d.msg, chan), BF16), VMEM((rows, n, 2 * chan, chan), F32)],
            in_specs=[aspec] * 5 + [vspec] * 7,
            out_specs=[vspec, vspec],
            scratch_shapes=[field, field, VMEM(w.shape, F32), raw, raw, mat, mat, mat, mat, stage, stage, spec, spec,
                            VMEM((4, n, d.msg, chan), BF16), VMEM((3, n, d.msg, chan), BF16), VMEM((4, nr, d.msg, chan), BF16),
                            VMEM((2, n, sl_rows, chan), BF16), VMEM((2, n, sl_rows, chan), BF16), VMEM((2, nr, sl_rows, chan), BF16),
                            dma(12), dma(6, n), dma(6, n), dma(6, nr), dma(6, nr), dma(6, nr),
                            dma(4), dma(4), dma(4, 4), dma(4, 4), dma(16), dma(16)],
            compiler_params=pltpu.CompilerParams(collective_id=0, has_side_effects=True, vmem_limit_bytes=44 * 1024 * 1024),
        )(f, dg, w, p_fwd, p_inv, perm, ah, al, bh, bl, sh, sl)
        df, dw = pl.pallas_call(
            functools.partial(final_kernel, d), name="final",
            out_shape=[jax.ShapeDtypeStruct((d.bt, lon, chan), F32), jax.ShapeDtypeStruct(full.shape, F32)],
            in_specs=[vspec, aspec, vspec, vspec, vspec], out_specs=[vspec, aspec],
            scratch_shapes=[field, stage, dma(2)],
            compiler_params=pltpu.CompilerParams(vmem_limit_bytes=16 * 1024 * 1024),
        )(recv4, dg, full, zh, zl)
        grad_field = df.reshape(batch, rows, lon, chan).transpose(0, 3, 1, 2)
        grad_wmix = dw.reshape(d.lat, chan, 2, chan).transpose(0, 1, 3, 2)
        return grad_field, grad_wmix

    return jax.shard_map(local_step, mesh=mesh, in_specs=(field_spec, field_spec, P(), P(), P()), out_specs=(field_spec, P('member', None, None, None)), check_vma=False)
```

```python
import functools
import math
import numpy as np
import jax
import jax.numpy as jnp
from jax import lax
from jax.experimental import pallas as pl
from jax.experimental.pallas import tpu as pltpu
from jax.sharding import PartitionSpec as P

MESH = pl.DeviceIdType.MESH
F32, BF16 = jnp.float32, jnp.bfloat16
VMEM = pltpu.VMEM


class Dims:
    def __init__(self, n, batch, chan, rows, lon):
        self.n = n
        self.side = math.isqrt(n // 2)
        self.nc = 2
        self.b, self.c, self.t, self.lon = batch // self.nc, chan, rows, lon
        self.lat = n * rows
        self.bt = self.b * rows
        self.msg = 2 * rows * self.bt
        self.lp = self.lat + 8
        self.ship_off = [self.b * j * (j + 1) for j in range(rows + 1)]


def split_const(mat):
    hi = mat.astype(jnp.bfloat16)
    lo = (mat - hi.astype(np.float64)).astype(jnp.bfloat16)
    return hi, lo


def dft_constants(d):
    m = np.arange(d.lat)
    ang = 2.0 * np.pi * np.outer(m, np.arange(d.lon)) / d.lon
    scale = 1.0 / math.sqrt(d.lon)
    ana = scale * np.concatenate([np.cos(ang), -np.sin(ang)])
    gain = np.where(m == 0, 1.0, 2.0)[:, None]
    ana2 = scale * np.concatenate([np.cos(ang) * gain, -np.sin(ang) * gain])
    syn = ana2.T
    syn2 = ana.T
    return [split_const(a) for a in (ana, ana2, syn, syn2)]


def perm_constant(d):
    t = np.arange(d.lat)
    tau = (t % d.t) * d.n + t // d.t
    mat = np.zeros((d.lat, d.lat))
    mat[t, tau] = 1.0
    return mat.astype(jnp.bfloat16)


def mm(a, b):
    return jnp.dot(a, b, preferred_element_type=F32)


def mm_nt(a, b):
    return lax.dot_general(a, b, (((1,), (1,)), ((), ())), preferred_element_type=F32)


def mm_tn(a, b):
    return lax.dot_general(a, b, (((0,), (0,)), ((), ())), preferred_element_type=F32)


def rnd(x):
    return x.astype(BF16).astype(F32)


class Torus:
    def __init__(self, d, me):
        side = d.side
        y, x, h = me // (2 * side), lax.rem(me // 2, side), lax.rem(me, 2)
        self.side, self.h = side, h
        self.ys = [lax.rem(y + i, side) * (2 * side) for i in range(side)]
        self.xs = [lax.rem(x + i, side) * 2 for i in range(side)]
        self.hs = [h, 1 - h]

    def at(self, dy, dx, dh):
        return self.ys[dy % self.side] + self.xs[dx % self.side] + self.hs[dh % 2]


def remote(src, dst, ssem, rsem, to):
    return pltpu.make_async_remote_copy(src_ref=src, dst_ref=dst, send_sem=ssem, recv_sem=rsem,
                                        device_id={"lat": to}, device_id_type=MESH)


class Exchange:
    def __init__(self, d, me, tor, send, recv, hold, sems):
        self.d, self.me, self.tor, self.send, self.recv, self.hold = d, me, tor, send, recv, hold
        self.ssem, self.rsem, self.hsem, self.fsem = [sems.at[i] for i in range(4)]
        side, half = d.side, d.side // 2
        self.half = half
        chips = [(dy, dx) for dy in range(side) for dx in range(side)]
        self.relayed = [o for o in chips if half in o]
        self.direct = [o + (1,) for o in chips if half not in o] + [o + (0,) for o in chips if o != (0, 0)]

    def hop(self, dy, dx):
        return -int(dy == self.half), -int(dx == self.half)

    def start(self):
        for i, (dy, dx) in enumerate(self.relayed):
            ry, rx = self.hop(dy, dx)
            to, via = self.tor.at(dy, dx, 1), self.tor.at(ry, rx, 0)
            remote(self.send.at[to], self.hold.at[i], self.ssem, self.hsem, via).start()
        for o in self.direct:
            to = self.tor.at(*o)
            remote(self.send.at[to], self.recv.at[self.me], self.ssem, self.rsem, to).start()

    def wait(self, ref, sem):
        pltpu.make_async_copy(ref, ref, sem).wait()

    def forward(self):
        self.wait(self.hold, self.hsem)
        for i, (dy, dx) in enumerate(self.relayed):
            ry, rx = self.hop(dy, dx)
            origin, to = self.tor.at(-ry, -rx, 0), self.tor.at(dy - ry, dx - rx, 1)
            remote(self.hold.at[i], self.recv.at[origin], self.fsem, self.rsem, to).start()

    def collect(self):
        self.recv[self.me] = self.send[self.me]
        self.wait(self.recv.at[0:self.d.n - 1], self.rsem)

    def drain(self):
        self.wait(self.send.at[0:self.d.n - 1], self.ssem)
        self.wait(self.hold, self.fsem)


def message_rows(d, s):
    return pl.ds(pl.multiple_of(s * d.msg, 8), d.msg)


def ring_rows(d, start):
    return pl.ds(start, d.n, stride=d.msg)


def put_modes(d, stage, y, bt, lanes):
    for rk in range(2 * d.t):
        stage[ring_rows(d, rk * d.bt + bt), :] = y[rk * d.n:(rk + 1) * d.n, lanes]


def get_modes(d, stage, bt):
    return jnp.concatenate([stage[ring_rows(d, rk * d.bt + bt), :] for rk in range(2 * d.t)], axis=0)


def analyse(x, hi, lo):
    xh = x.astype(BF16)
    xl = (x - xh.astype(F32)).astype(BF16)
    return mm(hi[...], xh) + mm(lo[...], xh) + mm(hi[...], xl)


def loop(count, body, unroll=1):
    def step(i, _):
        body(i)
        return 0
    lax.fori_loop(0, count, step, 0, unroll=unroll)


def lane_halves(d):
    return slice(0, d.c), slice(d.c, 2 * d.c)


def permuted(d, perm, p, out, outt):
    for k in range(d.t):
        pk = p[k].astype(BF16)
        out[k] = mm(pk, perm[...]).astype(BF16)
        outt[k] = mm_tn(perm[...], pk.T).astype(BF16)


def spec_at(d, r, k, b):
    return pl.multiple_of(((k * 2 + r) * d.b + b) * d.lp + d.n * k, 8)


def to_spectral(d, stage, spec, turn, p, sign):
    for k in range(d.t):
        low = d.n * k

        def body(b):
            x = jnp.concatenate([jnp.concatenate(
                [stage[ring_rows(d, (r * d.t + k) * d.bt + b * d.t + t), :] for t in range(d.t)], axis=0)
                for r in range(2)], axis=1)
            y = rnd(mm(p[k, low:, :], x.astype(BF16)))
            for r, half in enumerate(lane_halves(d)):
                spec[pl.ds(spec_at(d, r, k, b), d.lat - low), :] = y[:, half]
                turn[pl.ds(spec_at(d, 1 - r, k, b), d.lat - low), :] = y[:, half] * (sign if r == 0 else -sign)
        loop(d.b, body, d.b)


def from_spectral(d, spec, stage, pt):
    for k in range(d.t):
        low = d.n * k

        def body(b):
            x = jnp.concatenate([spec[pl.ds(spec_at(d, r, k, b), d.lat - low), :] for r in range(2)], axis=1).astype(BF16)
            y = mm(pt[k][:, low:], x)
            for r, half in enumerate(lane_halves(d)):
                for t in range(d.t):
                    stage[ring_rows(d, (r * d.t + k) * d.bt + b * d.t + t), :] = y[t * d.n:(t + 1) * d.n, half]
        loop(d.b, body, d.b)


def mix(d, spec, turn, out, w, ship, base, forward):
    for j in range(d.t):
        rows = 2 * d.b * (j + 1)

        def body(ll):
            l = d.n * j + ll
            at = pl.ds(l, rows, stride=d.lp)
            x = spec[at, :].astype(BF16)
            ship[ll, base + d.ship_off[j]:base + d.ship_off[j + 1], :] = x
            x2 = jnp.concatenate([x, turn[at, :].astype(BF16)], axis=1)
            if forward:
                y = mm_nt(x2, jnp.concatenate([w[l, :d.c, :], w[l, d.c:, :]], axis=1))
            else:
                y = mm(x2, w[l])
            out[at, :] = rnd(y)
        loop(d.n, body, 8)


def gelu_grad(values):
    cumulative = 0.5 * (1.0 + lax.erf(values * math.sqrt(0.5)))
    density = jnp.exp(-0.5 * values * values) * (1.0 / math.sqrt(2.0 * math.pi))
    return cumulative + values * density


def weights(d, a, dq, out, me):
    size = d.ship_off[-1]
    for j in range(d.t):
        y = 0.0
        for c in range(d.nc):
            at = slice(c * size + d.ship_off[j], c * size + d.ship_off[j + 1])
            groups = d.n * (j + 1)
            x = a[:, at, :].astype(F32).reshape(groups, 2 * d.b, d.c)
            turn = jnp.concatenate([-x[:, d.b:, :], x[:, :d.b, :]], axis=1)
            both = jnp.concatenate([x, turn], axis=2).reshape(groups * 2 * d.b, 2 * d.c)
            g = dq[:, at, :].astype(F32).reshape(groups * 2 * d.b, d.c)
            y = y + mm_tn(g.astype(BF16), both.astype(BF16))
        for r, half in enumerate(lane_halves(d)):
            out[j, me, pl.ds(r, d.c, stride=2), :] = y[:, half]


class Gather:
    def __init__(self, d, me, tor, full, ssem, r1, r2, rp):
        self.d, self.me, self.tor, self.full = d, me, tor, full
        self.ssem, self.r1, self.r2, self.rp = ssem, r1, r2, rp
        self.half = full.shape[2] // 2
        h, side = tor.h, tor.side
        self.first = [lax.select(h == 0, tor.xs[i], tor.ys[i]) for i in range(side)]
        self.second = [lax.select(h == 0, tor.ys[i], tor.xs[i]) for i in range(side)]

    def near(self, one, two):
        return self.first[one % self.d.side] + self.second[two % self.d.side] + self.tor.h

    def piece(self, block, part):
        if part is None:
            return self.full.at[:, block]
        return self.full.at[:, block, self.half * part:self.half * (part + 1), :]

    def start(self, block, part, rsem, to):
        ref = self.piece(block, part)
        remote(ref, ref, self.ssem, rsem, to).start()

    def arrive(self, block, part, rsem):
        ref = self.piece(block, part)
        pltpu.make_async_copy(ref, ref, rsem).wait()

    def run(self, between):
        near, r1, r2, rp = self.near, self.r1, self.r2, self.rp
        partner = self.tor.at(0, 0, 1)
        pos = [0, -1, 1, 2]
        p1, m1, p2, m2 = near(1, 0), near(-1, 0), near(0, 1), near(0, -1)
        group = [near(i, 0) for i in pos]

        def second(q):
            self.start(group[q], None, r2.at[q, 0], p2)
            self.start(group[q], None, r2.at[q, 1], m2)
            self.start(group[q], None, rp.at[q], partner)

        def relay(q):
            for i, (off, to) in enumerate(((-1, p2), (1, m2))):
                block = near(pos[q], off)
                self.arrive(block, None, r2.at[q, i])
                self.start(block, i, r2.at[q, 2 + i], to)
                self.start(block, None, rp.at[4 + 2 * q + i], partner)

        self.start(group[0], None, r1.at[0], p1)
        self.start(group[0], None, r1.at[1], m1)
        second(0)
        between()
        self.arrive(group[1], None, r1.at[0])
        self.start(group[1], 0, r1.at[2], p1)
        second(1)
        self.arrive(group[2], None, r1.at[1])
        self.start(group[2], 1, r1.at[3], m1)
        second(2)
        relay(0)
        self.arrive(group[3], 0, r1.at[2])
        self.arrive(group[3], 1, r1.at[3])
        second(3)
        for q in (1, 2, 3):
            relay(q)
        for q in range(4):
            block = near(pos[q], 2)
            for i in range(2):
                self.arrive(block, i, r2.at[q, 2 + i])
            self.start(block, None, rp.at[12 + q], partner)
        for i in range(16):
            self.arrive(partner, None, rp.at[i])
        every = self.full.at[:, 0:31]
        pltpu.make_async_copy(every, every, self.ssem).wait()


def main_kernel(d, f_h, dg_h, w_h, pf_h, pi_h, perm, ah, al, bh, bl, sh, sl, recv4, full,
                f, dg, w, pf, pi, pw, pwt, pv, pvt, stage, stage2, spec, turn, spec2, send, recv, hold, ship, shipr, shold,
                isem, esem, gsem, r1, r2, rp):
    me = lax.axis_index("lat")
    tor = Torus(d, me)
    bar = pltpu.get_barrier_semaphore()
    loads = [pltpu.make_async_copy(f_h.at[c * d.bt:(c + 1) * d.bt], f.at[c * d.bt:(c + 1) * d.bt], isem.at[c]) for c in range(d.nc)]
    small = []
    for k in range(d.t):
        small.append(pltpu.make_async_copy(pf_h.at[me + k * d.n], pf.at[k], isem.at[d.nc + 2 * k]))
        small.append(pltpu.make_async_copy(pi_h.at[me + k * d.n], pi.at[k], isem.at[d.nc + 2 * k + 1]))
    wloads = [pltpu.make_async_copy(w_h.at[j], full.at[j], isem.at[d.nc + 6 + j]) for j in range(d.t)]
    gload = pltpu.make_async_copy(dg_h, dg, isem.at[d.nc + 6 + d.t])
    for c in loads:
        c.start()

    def greet(k, _):
        pl.semaphore_signal(bar, inc=1, device_id={"lat": lax.rem(me + k, d.n)}, device_id_type=MESH)
        return 0
    lax.fori_loop(1, d.n, greet, 0)

    def exchange(e, snd, rcv, hld):
        return Exchange(d, me, tor, snd, rcv, hld, esem.at[e])

    ex = [[exchange(i * d.nc + c, send.at[i, c], recv.at[i, c] if i < 3 else recv4.at[c], hold.at[i, c])
           for c in range(d.nc)] for i in range(4)]
    ships = [exchange(4 * d.nc + i, ship.at[i], shipr.at[i], shold.at[i]) for i in range(2)]

    def dispatch(i, c, st):
        def fill(s):
            send[i, c, s] = st[message_rows(d, s), :].astype(BF16)
        loop(d.n, fill, 4)
        ex[i][c].start()

    def collect(i, c, st):
        ex[i][c].collect()

        def take(s):
            st[message_rows(d, s), :] = recv[i, c, s].astype(F32)
        loop(d.n, take, 4)

    for c in range(d.nc):
        loads[c].wait()
        if c == 0:
            for x in small + wloads + [gload]:
                x.start()

        def analysis_step(p):
            bt = c * d.bt + 2 * p
            y = analyse(jnp.concatenate([f[bt], f[bt + 1]], axis=1), ah, al)
            for u, half in enumerate(lane_halves(d)):
                put_modes(d, stage, y, 2 * p + u, half)
        loop(d.bt // 2, analysis_step, 3)
        if c == 0:
            pl.semaphore_wait(bar, d.n - 1)
        dispatch(0, c, stage)
    for x in small:
        x.wait()
    permuted(d, perm, pf, pw, pwt)
    permuted(d, perm, pi, pv, pvt)
    ex[0][0].forward()
    for j in range(d.t):
        wloads[j].wait()

        def prepare(ll):
            for r in range(2):
                w[d.n * j + ll, r * d.c:(r + 1) * d.c, :] = full[j, ll, pl.ds(r, d.c, stride=2), :].astype(BF16)
        loop(d.n, prepare, 4)

    for c in range(d.nc):
        collect(0, c, stage2)
        if c + 1 < d.nc:
            ex[0][c + 1].forward()
        to_spectral(d, stage2, spec, turn, pw, 1.0)
        mix(d, spec, turn, spec2, w, ship.at[0], c * d.ship_off[-1], True)
        from_spectral(d, spec2, stage, pvt)
        dispatch(1, c, stage)
    ships[0].start()
    gload.wait()
    ex[1][0].forward()
    for c in range(d.nc):
        collect(1, c, stage2)
        if c + 1 < d.nc:
            ex[1][c + 1].forward()

        def grid_step(p):
            bt = 2 * p
            at = c * d.bt + bt
            g = jnp.concatenate([get_modes(d, stage2, bt), get_modes(d, stage2, bt + 1)], axis=1).astype(BF16)
            h = mm(sh[...], g) + mm(sl[...], g)
            u = jnp.concatenate([dg[at], dg[at + 1]], axis=1) * gelu_grad(h)
            y = analyse(u, bh, bl)
            for i, half in enumerate(lane_halves(d)):
                put_modes(d, stage, y, bt + i, half)
        loop(d.bt // 2, grid_step, 2)
        dispatch(2, c, stage)
    ships[0].forward()
    ex[2][0].forward()
    for c in range(d.nc):
        collect(2, c, stage2)
        if c + 1 < d.nc:
            ex[2][c + 1].forward()
        to_spectral(d, stage2, spec, turn, pv, -1.0)
        mix(d, spec, turn, spec2, w, ship.at[1], c * d.ship_off[-1], False)
        if c + 1 == d.nc:
            ships[1].start()
        from_spectral(d, spec2, stage, pwt)
        dispatch(3, c, stage)
    ships[0].collect()
    ships[1].forward()
    ships[1].collect()
    weights(d, shipr.at[0], shipr.at[1], full, me)
    gather = Gather(d, me, tor, full, gsem.at[0], r1, r2, rp)

    def between():
        for e in ex[3]:
            e.forward()
    gather.run(between)
    for e in ex[3]:
        e.collect()
    for e in sum(ex, []) + ships:
        e.drain()


def final_kernel(d, got, dg_h, full, shi, slo, out, dw, dg, stage, sem):
    copy = pltpu.make_async_copy(full, dw, sem.at[0])
    load = pltpu.make_async_copy(dg_h, dg, sem.at[1])
    load.start()
    copy.start()
    for c in range(d.nc):
        def take(s):
            stage[message_rows(d, s), :] = got[c, s].astype(F32)
        loop(d.n, take, 2)
        if c == 0:
            load.wait()

        def body(p):
            bt = 2 * p
            at = c * d.bt + bt
            g = jnp.concatenate([get_modes(d, stage, bt), get_modes(d, stage, bt + 1)], axis=1).astype(BF16)
            y = mm(shi[...], g) + mm(slo[...], g)
            for i, half in enumerate(lane_halves(d)):
                out[at + i] = dg[at + i] + y[:, half]
        loop(d.bt // 2, body, 2)
    copy.wait()


def solution(mesh):
    n = mesh.shape['lat']
    field_spec = P('member', None, 'lat', None)

    def local_step(field_loc, grad_loc, p_fwd, p_inv, w_mix):
        batch, chan, rows, lon = field_loc.shape
        d = Dims(n, batch, chan, rows, lon)
        (ah, al), (bh, bl), (sh, sl), (zh, zl) = dft_constants(d)
        perm = perm_constant(d)
        f = field_loc.transpose(0, 2, 3, 1).reshape(batch * rows, lon, chan)
        dg = grad_loc.transpose(0, 2, 3, 1).reshape(batch * rows, lon, chan)
        w = w_mix.transpose(0, 1, 3, 2).reshape(rows, n, 2 * chan, chan)

        nr = 2 * d.side - 1
        sl_rows = d.nc * d.ship_off[-1]
        nc, ne = d.nc, 4 * d.nc + 2
        stage = VMEM((n * d.msg, chan), F32)
        spec = VMEM((2 * rows * d.b * d.lp, chan), F32)
        mat = VMEM((rows, d.lat, d.lat), BF16)
        raw = VMEM((rows, d.lat, d.lat), F32)
        field = VMEM(f.shape, F32)
        dma = lambda *s: pltpu.SemaphoreType.DMA(s)
        vspec = pl.BlockSpec(memory_space=VMEM)
        aspec = pl.BlockSpec(memory_space=pl.ANY)
        recv4, full = pl.pallas_call(
            functools.partial(main_kernel, d), name="main",
            out_shape=[VMEM((nc, n, d.msg, chan), BF16), VMEM((rows, n, 2 * chan, chan), F32)],
            in_specs=[aspec] * 5 + [vspec] * 7,
            out_specs=[vspec, vspec],
            scratch_shapes=[field, field, VMEM((d.lat, 2 * chan, chan), BF16), raw, raw, mat, mat, mat, mat, stage, stage, spec, spec, spec,
                            VMEM((4, nc, n, d.msg, chan), BF16), VMEM((3, nc, n, d.msg, chan), BF16), VMEM((4, nc, nr, d.msg, chan), BF16),
                            VMEM((2, n, sl_rows, chan), BF16), VMEM((2, n, sl_rows, chan), BF16), VMEM((2, nr, sl_rows, chan), BF16),
                            dma(nc + 7 + rows), dma(ne, 4), dma(1), dma(4), dma(4, 4), dma(16)],
            compiler_params=pltpu.CompilerParams(collective_id=0, has_side_effects=True, vmem_limit_bytes=38 * 1024 * 1024),
        )(f, dg, w, p_fwd, p_inv, perm, ah, al, bh, bl, sh, sl)
        df, dw = pl.pallas_call(
            functools.partial(final_kernel, d), name="final",
            out_shape=[jax.ShapeDtypeStruct(f.shape, F32), jax.ShapeDtypeStruct(full.shape, F32)],
            in_specs=[vspec, aspec, vspec, vspec, vspec], out_specs=[vspec, aspec],
            scratch_shapes=[field, stage, dma(2)],
            compiler_params=pltpu.CompilerParams(vmem_limit_bytes=16 * 1024 * 1024),
        )(recv4, dg, full, zh, zl)
        grad_field = df.reshape(batch, rows, lon, chan).transpose(0, 3, 1, 2)
        grad_wmix = dw.reshape(d.lat, chan, 2, chan).transpose(0, 1, 3, 2)
        return grad_field, grad_wmix

    return jax.shard_map(local_step, mesh=mesh, in_specs=(field_spec, field_spec, P(), P(), P()), out_specs=(field_spec, P('member', None, None, None)), check_vma=False)
```

```python
import functools
import math
import numpy as np
import jax
import jax.numpy as jnp
from jax import lax
from jax.experimental import pallas as pl
from jax.experimental.pallas import tpu as pltpu
from jax.sharding import PartitionSpec as P

MESH = pl.DeviceIdType.MESH
F32, BF16 = jnp.float32, jnp.bfloat16
VMEM = pltpu.VMEM


class Dims:
    def __init__(self, n, batch, chan, rows, lon):
        self.n = n
        self.side = math.isqrt(n // 2)
        self.nc = 2
        self.b, self.c, self.t, self.lon = batch // self.nc, chan, rows, lon
        self.lat = n * rows
        self.bt = self.b * rows
        self.msg = 2 * rows * self.bt
        self.lp = self.lat + 8
        self.ship_off = [self.b * j * (j + 1) for j in range(rows + 1)]


def split_const(mat):
    hi = mat.astype(jnp.bfloat16)
    lo = (mat - hi.astype(np.float64)).astype(jnp.bfloat16)
    return hi, lo


def dft_constants(d):
    m = np.arange(d.lat)
    ang = 2.0 * np.pi * np.outer(m, np.arange(d.lon)) / d.lon
    scale = 1.0 / math.sqrt(d.lon)
    ana = scale * np.concatenate([np.cos(ang), -np.sin(ang)])
    gain = np.where(m == 0, 1.0, 2.0)[:, None]
    ana2 = scale * np.concatenate([np.cos(ang) * gain, -np.sin(ang) * gain])
    syn = ana2.T
    syn2 = ana.T
    return [split_const(a) for a in (ana, ana2, syn, syn2)]


def perm_constant(d):
    t = np.arange(d.lat)
    tau = (t % d.t) * d.n + t // d.t
    mat = np.zeros((d.lat, d.lat))
    mat[t, tau] = 1.0
    return mat.astype(jnp.bfloat16)


def mm(a, b):
    return jnp.dot(a, b, preferred_element_type=F32)


def mm_nt(a, b):
    return lax.dot_general(a, b, (((1,), (1,)), ((), ())), preferred_element_type=F32)


def mm_tn(a, b):
    return lax.dot_general(a, b, (((0,), (0,)), ((), ())), preferred_element_type=F32)


def rnd(x):
    return x.astype(BF16).astype(F32)


class Torus:
    def __init__(self, d, me):
        side = d.side
        y, x, h = me // (2 * side), lax.rem(me // 2, side), lax.rem(me, 2)
        self.side, self.h = side, h
        self.ys = [lax.rem(y + i, side) * (2 * side) for i in range(side)]
        self.xs = [lax.rem(x + i, side) * 2 for i in range(side)]
        self.hs = [h, 1 - h]

    def at(self, dy, dx, dh):
        return self.ys[dy % self.side] + self.xs[dx % self.side] + self.hs[dh % 2]


def remote(src, dst, ssem, rsem, to):
    return pltpu.make_async_remote_copy(src_ref=src, dst_ref=dst, send_sem=ssem, recv_sem=rsem,
                                        device_id={"lat": to}, device_id_type=MESH)


class Exchange:
    def __init__(self, d, me, tor, send, recv, sems):
        self.d, self.me, self.tor, self.send, self.recv = d, me, tor, send, recv
        self.ssem, self.rsem = sems.at[0], sems.at[1]
        self.offsets = [(dy, dx, dh) for dy in range(d.side) for dx in range(d.side) for dh in range(2)][1:]

    def start(self):
        for o in self.offsets:
            to = self.tor.at(*o)
            remote(self.send.at[to], self.recv.at[self.me], self.ssem, self.rsem, to).start()

    def wait(self, ref, sem):
        pltpu.make_async_copy(ref, ref, sem).wait()

    def collect(self):
        self.recv[self.me] = self.send[self.me]
        self.wait(self.recv.at[0:self.d.n - 1], self.rsem)

    def drain(self):
        self.wait(self.send.at[0:self.d.n - 1], self.ssem)


def message_rows(d, s):
    return pl.ds(pl.multiple_of(s * d.msg, 8), d.msg)


def ring_rows(d, start):
    return pl.ds(start, d.n, stride=d.msg)


def put_modes(d, stage, y, bt, lanes):
    for rk in range(2 * d.t):
        stage[ring_rows(d, rk * d.bt + bt), :] = y[rk * d.n:(rk + 1) * d.n, lanes]


def get_modes(d, stage, bt):
    return jnp.concatenate([stage[ring_rows(d, rk * d.bt + bt), :] for rk in range(2 * d.t)], axis=0)


def analyse(x, hi, lo):
    xh = x.astype(BF16)
    xl = (x - xh.astype(F32)).astype(BF16)
    return mm(hi[...], xh) + mm(lo[...], xh) + mm(hi[...], xl)


def loop(count, body, unroll=1):
    def step(i, _):
        body(i)
        return 0
    lax.fori_loop(0, count, step, 0, unroll=unroll)


def lane_halves(d):
    return slice(0, d.c), slice(d.c, 2 * d.c)


def permuted(d, perm, p, out, outt):
    for k in range(d.t):
        pk = p[k].astype(BF16)
        out[k] = mm(pk, perm[...]).astype(BF16)
        outt[k] = mm_tn(perm[...], pk.T).astype(BF16)


def spec_at(d, r, k, b):
    return pl.multiple_of(((k * 2 + r) * d.b + b) * d.lp + d.n * k, 8)


def to_spectral(d, stage, spec, turn, p, sign):
    for k in range(d.t):
        low = d.n * k

        def body(b):
            x = jnp.concatenate([jnp.concatenate(
                [stage[ring_rows(d, (r * d.t + k) * d.bt + b * d.t + t), :] for t in range(d.t)], axis=0)
                for r in range(2)], axis=1)
            y = rnd(mm(p[k, low:, :], x.astype(BF16)))
            for r, half in enumerate(lane_halves(d)):
                spec[pl.ds(spec_at(d, r, k, b), d.lat - low), :] = y[:, half]
                turn[pl.ds(spec_at(d, 1 - r, k, b), d.lat - low), :] = y[:, half] * (sign if r == 0 else -sign)
        loop(d.b, body, d.b)


def from_spectral(d, spec, stage, pt):
    for k in range(d.t):
        low = d.n * k

        def body(b):
            x = jnp.concatenate([spec[pl.ds(spec_at(d, r, k, b), d.lat - low), :] for r in range(2)], axis=1).astype(BF16)
            y = mm(pt[k][:, low:], x)
            for r, half in enumerate(lane_halves(d)):
                for t in range(d.t):
                    stage[ring_rows(d, (r * d.t + k) * d.bt + b * d.t + t), :] = y[t * d.n:(t + 1) * d.n, half]
        loop(d.b, body, d.b)


def mix(d, spec, turn, out, w, ship, base, forward):
    for j in range(d.t):
        rows = 2 * d.b * (j + 1)

        def body(ll):
            l = d.n * j + ll
            at = pl.ds(l, rows, stride=d.lp)
            x = spec[at, :].astype(BF16)
            ship[ll, base + d.ship_off[j]:base + d.ship_off[j + 1], :] = x
            x2 = jnp.concatenate([x, turn[at, :].astype(BF16)], axis=1)
            if forward:
                y = mm_nt(x2, jnp.concatenate([w[l, :d.c, :], w[l, d.c:, :]], axis=1))
            else:
                y = mm(x2, w[l])
            out[at, :] = rnd(y)
        loop(d.n, body, 8)


def gelu_grad(values):
    cumulative = 0.5 * (1.0 + lax.erf(values * math.sqrt(0.5)))
    density = jnp.exp(-0.5 * values * values) * (1.0 / math.sqrt(2.0 * math.pi))
    return cumulative + values * density


def weights(d, a, dq, out, me):
    size = d.ship_off[-1]
    for j in range(d.t):
        y = 0.0
        for c in range(d.nc):
            at = slice(c * size + d.ship_off[j], c * size + d.ship_off[j + 1])
            groups = d.n * (j + 1)
            x = a[:, at, :].astype(F32).reshape(groups, 2 * d.b, d.c)
            turn = jnp.concatenate([-x[:, d.b:, :], x[:, :d.b, :]], axis=1)
            both = jnp.concatenate([x, turn], axis=2).reshape(groups * 2 * d.b, 2 * d.c)
            g = dq[:, at, :].astype(F32).reshape(groups * 2 * d.b, d.c)
            y = y + mm_tn(g.astype(BF16), both.astype(BF16))
        for r, half in enumerate(lane_halves(d)):
            out[j, me, pl.ds(r, d.c, stride=2), :] = y[:, half]


class Gather:
    def __init__(self, d, me, tor, full, ssem, r1, r2, rp):
        self.d, self.me, self.tor, self.full = d, me, tor, full
        self.ssem, self.r1, self.r2, self.rp = ssem, r1, r2, rp
        self.half = full.shape[2] // 2
        h, side = tor.h, tor.side
        self.first = [lax.select(h == 0, tor.xs[i], tor.ys[i]) for i in range(side)]
        self.second = [lax.select(h == 0, tor.ys[i], tor.xs[i]) for i in range(side)]

    def near(self, one, two):
        return self.first[one % self.d.side] + self.second[two % self.d.side] + self.tor.h

    def piece(self, block, part):
        if part is None:
            return self.full.at[:, block]
        return self.full.at[:, block, self.half * part:self.half * (part + 1), :]

    def start(self, block, part, rsem, to):
        ref = self.piece(block, part)
        remote(ref, ref, self.ssem, rsem, to).start()

    def arrive(self, block, part, rsem):
        ref = self.piece(block, part)
        pltpu.make_async_copy(ref, ref, rsem).wait()

    def run(self):
        near, r1, r2, rp = self.near, self.r1, self.r2, self.rp
        partner = self.tor.at(0, 0, 1)
        pos = [0, -1, 1, 2]
        p1, m1, p2, m2 = near(1, 0), near(-1, 0), near(0, 1), near(0, -1)
        group = [near(i, 0) for i in pos]

        def second(q):
            self.start(group[q], None, r2.at[q, 0], p2)
            self.start(group[q], None, r2.at[q, 1], m2)
            self.start(group[q], None, rp.at[q], partner)

        def relay(q):
            for i, (off, to) in enumerate(((-1, p2), (1, m2))):
                block = near(pos[q], off)
                self.arrive(block, None, r2.at[q, i])
                self.start(block, i, r2.at[q, 2 + i], to)
                self.start(block, None, rp.at[4 + 2 * q + i], partner)

        self.start(group[0], None, r1.at[0], p1)
        self.start(group[0], None, r1.at[1], m1)
        second(0)
        self.arrive(group[1], None, r1.at[0])
        self.start(group[1], 0, r1.at[2], p1)
        second(1)
        self.arrive(group[2], None, r1.at[1])
        self.start(group[2], 1, r1.at[3], m1)
        second(2)
        relay(0)
        self.arrive(group[3], 0, r1.at[2])
        self.arrive(group[3], 1, r1.at[3])
        second(3)
        for q in (1, 2, 3):
            relay(q)
        for q in range(4):
            block = near(pos[q], 2)
            for i in range(2):
                self.arrive(block, i, r2.at[q, 2 + i])
            self.start(block, None, rp.at[12 + q], partner)
        for i in range(16):
            self.arrive(partner, None, rp.at[i])
        every = self.full.at[:, 0:31]
        pltpu.make_async_copy(every, every, self.ssem).wait()


def main_kernel(d, f_h, dg_h, w_h, pf_h, pi_h, perm_h, dft_h, recv4, full,
                perm, dft, f, dg, w, pf, pi, pw, pwt, pv, pvt, stage, stage2, spec, turn, spec2, send, recv, ship, shipr,
                isem, esem, gsem, r1, r2, rp):
    me = lax.axis_index("lat")
    tor = Torus(d, me)
    bar = pltpu.get_barrier_semaphore()
    loads = [pltpu.make_async_copy(f_h.at[c * d.bt:(c + 1) * d.bt], f.at[c * d.bt:(c + 1) * d.bt], isem.at[c]) for c in range(d.nc)]
    ah, al, bh, bl, sh, sl = [dft.at[i] for i in range(6)]
    tables = pltpu.make_async_copy(dft_h, dft, isem.at[d.nc + 7 + d.t])
    small = [pltpu.make_async_copy(perm_h, perm, isem.at[d.nc + 8 + d.t])]
    for k in range(d.t):
        small.append(pltpu.make_async_copy(pf_h.at[me + k * d.n], pf.at[k], isem.at[d.nc + 2 * k]))
        small.append(pltpu.make_async_copy(pi_h.at[me + k * d.n], pi.at[k], isem.at[d.nc + 2 * k + 1]))
    wloads = [pltpu.make_async_copy(w_h.at[j], full.at[j], isem.at[d.nc + 6 + j]) for j in range(d.t)]
    gload = pltpu.make_async_copy(dg_h, dg, isem.at[d.nc + 6 + d.t])
    for c in loads[:1] + [tables] + loads[1:]:
        c.start()

    def greet(k, _):
        pl.semaphore_signal(bar, inc=1, device_id={"lat": lax.rem(me + k, d.n)}, device_id_type=MESH)
        return 0
    lax.fori_loop(1, d.n, greet, 0)

    def exchange(e, snd, rcv):
        return Exchange(d, me, tor, snd, rcv, esem.at[e])

    ex = [[exchange(i * d.nc + c, send.at[i, c], recv.at[i, c] if i < 3 else recv4.at[c])
           for c in range(d.nc)] for i in range(4)]
    ships = [exchange(4 * d.nc + i, ship.at[i], shipr.at[i]) for i in range(2)]

    def dispatch(i, c, st):
        def fill(s):
            send[i, c, s] = st[message_rows(d, s), :].astype(BF16)
        loop(d.n, fill, 4)
        ex[i][c].start()

    def collect(i, c, st):
        ex[i][c].collect()

        def take(s):
            st[message_rows(d, s), :] = recv[i, c, s].astype(F32)
        loop(d.n, take, 4)

    for c in range(d.nc):
        loads[c].wait()
        if c == 0:
            tables.wait()
            for x in small + wloads + [gload]:
                x.start()

        def analysis_step(p):
            bt = c * d.bt + 2 * p
            y = analyse(jnp.concatenate([f[bt], f[bt + 1]], axis=1), ah, al)
            for u, half in enumerate(lane_halves(d)):
                put_modes(d, stage, y, 2 * p + u, half)
        loop(d.bt // 2, analysis_step, 3)
        if c == 0:
            pl.semaphore_wait(bar, d.n - 1)
        dispatch(0, c, stage)
    for x in small:
        x.wait()
    permuted(d, perm, pf, pw, pwt)
    permuted(d, perm, pi, pv, pvt)
    for j in range(d.t):
        wloads[j].wait()

        def prepare(ll):
            for r in range(2):
                w[d.n * j + ll, r * d.c:(r + 1) * d.c, :] = full[j, ll, pl.ds(r, d.c, stride=2), :].astype(BF16)
        loop(d.n, prepare, 4)

    for c in range(d.nc):
        collect(0, c, stage2)
        to_spectral(d, stage2, spec, turn, pw, 1.0)
        mix(d, spec, turn, spec2, w, ship.at[0], c * d.ship_off[-1], True)
        from_spectral(d, spec2, stage, pvt)
        dispatch(1, c, stage)
    ships[0].start()
    gload.wait()
    for c in range(d.nc):
        collect(1, c, stage2)

        def grid_step(p):
            bt = 2 * p
            at = c * d.bt + bt
            g = jnp.concatenate([get_modes(d, stage2, bt), get_modes(d, stage2, bt + 1)], axis=1).astype(BF16)
            h = mm(sh[...], g) + mm(sl[...], g)
            u = jnp.concatenate([dg[at], dg[at + 1]], axis=1) * gelu_grad(h)
            y = analyse(u, bh, bl)
            for i, half in enumerate(lane_halves(d)):
                put_modes(d, stage, y, bt + i, half)
        loop(d.bt // 2, grid_step, 2)
        dispatch(2, c, stage)
    for c in range(d.nc):
        collect(2, c, stage2)
        to_spectral(d, stage2, spec, turn, pv, -1.0)
        mix(d, spec, turn, spec2, w, ship.at[1], c * d.ship_off[-1], False)
        if c + 1 == d.nc:
            ships[1].start()
        from_spectral(d, spec2, stage, pwt)
        dispatch(3, c, stage)
    ships[0].collect()
    ships[1].collect()
    weights(d, shipr.at[0], shipr.at[1], full, me)
    gather = Gather(d, me, tor, full, gsem.at[0], r1, r2, rp)

    gather.run()
    for e in ex[3]:
        e.collect()
    for e in sum(ex, []) + ships:
        e.drain()


def final_kernel(d, got, dg_h, full, dft_h, out, dw, dg, stage, dft, sem):
    copy = pltpu.make_async_copy(full, dw, sem.at[0])
    load = pltpu.make_async_copy(dg_h, dg, sem.at[1])
    tables = pltpu.make_async_copy(dft_h, dft, sem.at[2])
    tables.start()
    load.start()
    copy.start()
    shi, slo = dft.at[0], dft.at[1]
    for c in range(d.nc):
        def take(s):
            stage[message_rows(d, s), :] = got[c, s].astype(F32)
        loop(d.n, take, 2)
        if c == 0:
            tables.wait()
            load.wait()

        def body(p):
            bt = 2 * p
            at = c * d.bt + bt
            g = jnp.concatenate([get_modes(d, stage, bt), get_modes(d, stage, bt + 1)], axis=1).astype(BF16)
            y = mm(shi[...], g) + mm(slo[...], g)
            for i, half in enumerate(lane_halves(d)):
                out[at + i] = dg[at + i] + y[:, half]
        loop(d.bt // 2, body, 2)
    copy.wait()


def solution(mesh):
    n = mesh.shape['lat']
    field_spec = P('member', None, 'lat', None)

    def local_step(field_loc, grad_loc, p_fwd, p_inv, w_mix):
        batch, chan, rows, lon = field_loc.shape
        d = Dims(n, batch, chan, rows, lon)
        tables = np.stack([m for pair in dft_constants(d) for m in pair])
        perm = perm_constant(d)
        f = field_loc.transpose(0, 2, 3, 1).reshape(batch * rows, lon, chan)
        dg = grad_loc.transpose(0, 2, 3, 1).reshape(batch * rows, lon, chan)
        w = w_mix.transpose(0, 1, 3, 2).reshape(rows, n, 2 * chan, chan)

        sl_rows = d.nc * d.ship_off[-1]
        nc, ne = d.nc, 4 * d.nc + 2
        stage = VMEM((n * d.msg, chan), F32)
        spec = VMEM((2 * rows * d.b * d.lp, chan), F32)
        mat = VMEM((rows, d.lat, d.lat), BF16)
        raw = VMEM((rows, d.lat, d.lat), F32)
        field = VMEM(f.shape, F32)
        dma = lambda *s: pltpu.SemaphoreType.DMA(s)
        vspec = pl.BlockSpec(memory_space=VMEM)
        hspec = pl.BlockSpec(memory_space=pltpu.HBM)
        recv4, full = pl.pallas_call(
            functools.partial(main_kernel, d), name="main",
            out_shape=[VMEM((nc, n, d.msg, chan), BF16), VMEM((rows, n, 2 * chan, chan), F32)],
            in_specs=[hspec] * 7,
            out_specs=[vspec, vspec],
            scratch_shapes=[VMEM(perm.shape, BF16), VMEM(tables[:6].shape, BF16), field, field, VMEM((d.lat, 2 * chan, chan), BF16), raw, raw, mat, mat, mat, mat, stage, stage, spec, spec, spec,
                            VMEM((4, nc, n, d.msg, chan), BF16), VMEM((3, nc, n, d.msg, chan), BF16),
                            VMEM((2, n, sl_rows, chan), BF16), VMEM((2, n, sl_rows, chan), BF16),
                            dma(nc + 9 + rows), dma(ne, 2), dma(1), dma(4), dma(4, 4), dma(16)],
            compiler_params=pltpu.CompilerParams(collective_id=0, has_side_effects=True, vmem_limit_bytes=50 * 1024 * 1024),
        )(f, dg, w, p_fwd, p_inv, perm, tables[:6])
        df, dw = pl.pallas_call(
            functools.partial(final_kernel, d), name="final",
            out_shape=[jax.ShapeDtypeStruct(f.shape, F32), jax.ShapeDtypeStruct(full.shape, F32)],
            in_specs=[vspec, hspec, vspec, hspec], out_specs=[vspec, hspec],
            scratch_shapes=[field, stage, VMEM(tables[6:].shape, BF16), dma(3)],
            compiler_params=pltpu.CompilerParams(vmem_limit_bytes=50 * 1024 * 1024),
        )(recv4, dg, full, tables[6:])
        grad_field = df.reshape(batch, rows, lon, chan).transpose(0, 3, 1, 2)
        grad_wmix = dw.reshape(d.lat, chan, 2, chan).transpose(0, 1, 3, 2)
        return grad_field, grad_wmix

    return jax.shard_map(local_step, mesh=mesh, in_specs=(field_spec, field_spec, P(), P(), P()), out_specs=(field_spec, P('member', None, None, None)), check_vma=False)
```

```python
import functools
import math
import numpy as np
import jax
import jax.numpy as jnp
from jax import lax
from jax.experimental import pallas as pl
from jax.experimental.pallas import tpu as pltpu
from jax.sharding import PartitionSpec as P

MESH = pl.DeviceIdType.MESH
F32, BF16 = jnp.float32, jnp.bfloat16
VMEM = pltpu.VMEM


class Dims:
    def __init__(self, n, batch, chan, rows, lon):
        self.n = n
        self.side = math.isqrt(n // 2)
        self.nc = 2
        self.b, self.c, self.t, self.lon = batch // self.nc, chan, rows, lon
        self.lat = n * rows
        self.bt = self.b * rows
        self.msg = 2 * rows * self.bt
        self.lp = self.lat + 8
        self.ship_off = [self.b * j * (j + 1) for j in range(rows + 1)]


def split_const(mat):
    hi = mat.astype(jnp.bfloat16)
    lo = (mat - hi.astype(np.float64)).astype(jnp.bfloat16)
    return hi, lo


def dft_constants(d):
    m = np.arange(d.lat)
    ang = 2.0 * np.pi * np.outer(m, np.arange(d.lon)) / d.lon
    scale = 1.0 / math.sqrt(d.lon)
    ana = scale * np.concatenate([np.cos(ang), -np.sin(ang)])
    gain = np.where(m == 0, 1.0, 2.0)[:, None]
    ana2 = scale * np.concatenate([np.cos(ang) * gain, -np.sin(ang) * gain])
    syn = ana2.T
    syn2 = ana.T
    return [split_const(a) for a in (ana, ana2, syn, syn2)]


def perm_constant(d):
    t = np.arange(d.lat)
    tau = (t % d.t) * d.n + t // d.t
    mat = np.zeros((d.lat, d.lat))
    mat[t, tau] = 1.0
    return mat.astype(jnp.bfloat16)


def mm(a, b):
    return jnp.dot(a, b, preferred_element_type=F32)


def mm_nt(a, b):
    return lax.dot_general(a, b, (((1,), (1,)), ((), ())), preferred_element_type=F32)


def mm_tn(a, b):
    return lax.dot_general(a, b, (((0,), (0,)), ((), ())), preferred_element_type=F32)


def rnd(x):
    return x.astype(BF16).astype(F32)


class Torus:
    def __init__(self, d, me):
        side = d.side
        y, x, h = me // (2 * side), lax.rem(me // 2, side), lax.rem(me, 2)
        self.side, self.h = side, h
        self.ys = [lax.rem(y + i, side) * (2 * side) for i in range(side)]
        self.xs = [lax.rem(x + i, side) * 2 for i in range(side)]
        self.hs = [h, 1 - h]

    def at(self, dy, dx, dh):
        return self.ys[dy % self.side] + self.xs[dx % self.side] + self.hs[dh % 2]


def remote(src, dst, ssem, rsem, to):
    return pltpu.make_async_remote_copy(src_ref=src, dst_ref=dst, send_sem=ssem, recv_sem=rsem,
                                        device_id={"lat": to}, device_id_type=MESH)


class Exchange:
    def __init__(self, d, me, tor, send, recv, sems):
        self.d, self.me, self.tor, self.send, self.recv = d, me, tor, send, recv
        self.ssem, self.rsem = sems.at[0], sems.at[1]
        self.offsets = [(dy, dx, dh) for dy in range(d.side) for dx in range(d.side) for dh in range(2)][1:]

    def start(self):
        for o in self.offsets:
            to = self.tor.at(*o)
            remote(self.send.at[to], self.recv.at[self.me], self.ssem, self.rsem, to).start()

    def wait(self, ref, sem):
        pltpu.make_async_copy(ref, ref, sem).wait()

    def collect(self):
        self.recv[self.me] = self.send[self.me]
        self.wait(self.recv.at[0:self.d.n - 1], self.rsem)

    def drain(self):
        self.wait(self.send.at[0:self.d.n - 1], self.ssem)


def message_rows(d, s):
    return pl.ds(pl.multiple_of(s * d.msg, 8), d.msg)


def ring_rows(d, start):
    return pl.ds(start, d.n, stride=d.msg)


def put_modes(d, stage, y, bt, lanes):
    for rk in range(2 * d.t):
        stage[ring_rows(d, rk * d.bt + bt), :] = y[rk * d.n:(rk + 1) * d.n, lanes]


def get_modes(d, stage, bt):
    return jnp.concatenate([stage[ring_rows(d, rk * d.bt + bt), :] for rk in range(2 * d.t)], axis=0)


def analyse(x, hi, lo):
    xh = x.astype(BF16)
    xl = (x - xh.astype(F32)).astype(BF16)
    return mm(hi[...], xh) + mm(lo[...], xh) + mm(hi[...], xl)


def loop(count, body, unroll=1):
    def step(i, _):
        body(i)
        return 0
    lax.fori_loop(0, count, step, 0, unroll=unroll)


def lane_halves(d):
    return slice(0, d.c), slice(d.c, 2 * d.c)


def permuted(d, perm, p, out, outt):
    for k in range(d.t):
        pk = p[k].astype(BF16)
        out[k] = mm(pk, perm[...]).astype(BF16)
        outt[k] = mm_tn(perm[...], pk.T).astype(BF16)


def spec_at(d, r, k, b):
    return pl.multiple_of(((k * 2 + r) * d.b + b) * d.lp + d.n * k, 8)


def to_spectral(d, stage, spec, turn, p, sign):
    for k in range(d.t):
        low = d.n * k

        def body(b):
            x = jnp.concatenate([jnp.concatenate(
                [stage[ring_rows(d, (r * d.t + k) * d.bt + b * d.t + t), :] for t in range(d.t)], axis=0)
                for r in range(2)], axis=1)
            y = rnd(mm(p[k, low:, :], x.astype(BF16)))
            for r, half in enumerate(lane_halves(d)):
                spec[pl.ds(spec_at(d, r, k, b), d.lat - low), :] = y[:, half]
                turn[pl.ds(spec_at(d, 1 - r, k, b), d.lat - low), :] = y[:, half] * (sign if r == 0 else -sign)
        loop(d.b, body, d.b)


def from_spectral(d, spec, stage, pt):
    for k in range(d.t):
        low = d.n * k

        def body(b):
            x = jnp.concatenate([spec[pl.ds(spec_at(d, r, k, b), d.lat - low), :] for r in range(2)], axis=1).astype(BF16)
            y = mm(pt[k][:, low:], x)
            for r, half in enumerate(lane_halves(d)):
                for t in range(d.t):
                    stage[ring_rows(d, (r * d.t + k) * d.bt + b * d.t + t), :] = y[t * d.n:(t + 1) * d.n, half]
        loop(d.b, body, d.b)


def extract(d, spec, ship):
    for j in range(d.t):
        def body(ll):
            ship[ll, d.ship_off[j]:d.ship_off[j + 1], :] = spec[pl.ds(d.n * j + ll, 2 * d.b * (j + 1), stride=d.lp), :].astype(BF16)
        loop(d.n, body, 8)


def mix(d, spec, turn, out, w, forward):
    for j in range(d.t):
        rows = 2 * d.b * (j + 1)

        def body(ll):
            l = d.n * j + ll
            at = pl.ds(l, rows, stride=d.lp)
            x = spec[at, :].astype(BF16)
            x2 = jnp.concatenate([x, turn[at, :].astype(BF16)], axis=1)
            if forward:
                y = mm_nt(x2, jnp.concatenate([w[l, :d.c, :], w[l, d.c:, :]], axis=1))
            else:
                y = mm(x2, w[l])
            out[at, :] = rnd(y)
        loop(d.n, body, 8)


def gelu_grad(values):
    cumulative = 0.5 * (1.0 + lax.erf(values * math.sqrt(0.5)))
    density = jnp.exp(-0.5 * values * values) * (1.0 / math.sqrt(2.0 * math.pi))
    return cumulative + values * density


def weights(d, a, dq):
    parts = []
    for j in range(d.t):
        at = slice(d.ship_off[j], d.ship_off[j + 1])
        groups = d.n * (j + 1)
        x = a[:, at, :].astype(F32).reshape(groups, 2 * d.b, d.c)
        turn = jnp.concatenate([-x[:, d.b:, :], x[:, :d.b, :]], axis=1)
        both = jnp.concatenate([x, turn], axis=2).reshape(groups * 2 * d.b, 2 * d.c)
        g = dq[:, at, :].astype(F32).reshape(groups * 2 * d.b, d.c)
        parts.append(mm_tn(g.astype(BF16), both.astype(BF16)))
    return parts


class Gather:
    def __init__(self, d, me, tor, full, ssem, r1, r2, rp):
        self.d, self.me, self.tor, self.full = d, me, tor, full
        self.ssem, self.r1, self.r2, self.rp = ssem, r1, r2, rp
        self.half = full.shape[2] // 2
        h, side = tor.h, tor.side
        self.first = [lax.select(h == 0, tor.xs[i], tor.ys[i]) for i in range(side)]
        self.second = [lax.select(h == 0, tor.ys[i], tor.xs[i]) for i in range(side)]

    def near(self, one, two):
        return self.first[one % self.d.side] + self.second[two % self.d.side] + self.tor.h

    def piece(self, block, part):
        if part is None:
            return self.full.at[:, block]
        return self.full.at[:, block, self.half * part:self.half * (part + 1), :]

    def start(self, block, part, rsem, to):
        ref = self.piece(block, part)
        remote(ref, ref, self.ssem, rsem, to).start()

    def arrive(self, block, part, rsem):
        ref = self.piece(block, part)
        pltpu.make_async_copy(ref, ref, rsem).wait()

    def run(self, tasks):
        near, r1, r2, rp = self.near, self.r1, self.r2, self.rp
        partner = self.tor.at(0, 0, 1)
        pos = [0, -1, 1, 2]
        p1, m1, p2, m2 = near(1, 0), near(-1, 0), near(0, 1), near(0, -1)
        group = [near(i, 0) for i in pos]

        def second(q):
            self.start(group[q], None, r2.at[q, 0], p2)
            self.start(group[q], None, r2.at[q, 1], m2)
            self.start(group[q], None, rp.at[q], partner)

        def relay(q):
            for i, (off, to) in enumerate(((-1, p2), (1, m2))):
                block = near(pos[q], off)
                self.arrive(block, None, r2.at[q, i])
                self.start(block, i, r2.at[q, 2 + i], to)
                self.start(block, None, rp.at[4 + 2 * q + i], partner)

        self.start(group[0], None, r1.at[0], p1)
        self.start(group[0], None, r1.at[1], m1)
        second(0)
        tasks[0]()
        self.arrive(group[1], None, r1.at[0])
        self.start(group[1], 0, r1.at[2], p1)
        second(1)
        self.arrive(group[2], None, r1.at[1])
        self.start(group[2], 1, r1.at[3], m1)
        second(2)
        tasks[1]()
        relay(0)
        self.arrive(group[3], 0, r1.at[2])
        self.arrive(group[3], 1, r1.at[3])
        second(3)
        for q in (1, 2, 3):
            relay(q)
        for q in range(4):
            block = near(pos[q], 2)
            for i in range(2):
                self.arrive(block, i, r2.at[q, 2 + i])
            self.start(block, None, rp.at[12 + q], partner)
        for i in range(16):
            self.arrive(partner, None, rp.at[i])
        every = self.full.at[:, 0:31]
        pltpu.make_async_copy(every, every, self.ssem).wait()


def main_kernel(d, f_h, dg_h, w_h, pf_h, pi_h, perm_h, dft_h, df, full,
                perm, dft, wsum, f, dg, w, pf, pi, pw, pwt, pv, pvt, stage, stage2, spec, turn, spec2, send, recv, ship, shipr,
                isem, esem, gsem, r1, r2, rp):
    me = lax.axis_index("lat")
    tor = Torus(d, me)
    bar = pltpu.get_barrier_semaphore()
    loads = [pltpu.make_async_copy(f_h.at[c * d.bt:(c + 1) * d.bt], f.at[c * d.bt:(c + 1) * d.bt], isem.at[c]) for c in range(d.nc)]
    ah, al, bh, bl, sh, sl, zh, zl = [dft.at[i] for i in range(8)]
    tables = pltpu.make_async_copy(dft_h, dft, isem.at[d.nc + 7 + d.t])
    small = [pltpu.make_async_copy(perm_h, perm, isem.at[d.nc + 8 + d.t])]
    for k in range(d.t):
        small.append(pltpu.make_async_copy(pf_h.at[me + k * d.n], pf.at[k], isem.at[d.nc + 2 * k]))
        small.append(pltpu.make_async_copy(pi_h.at[me + k * d.n], pi.at[k], isem.at[d.nc + 2 * k + 1]))
    wloads = [pltpu.make_async_copy(w_h.at[j], full.at[j], isem.at[d.nc + 6 + j]) for j in range(d.t)]
    gload = pltpu.make_async_copy(dg_h, dg, isem.at[d.nc + 6 + d.t])
    for c in loads[:1] + [tables] + loads[1:]:
        c.start()

    def greet(k, _):
        pl.semaphore_signal(bar, inc=1, device_id={"lat": lax.rem(me + k, d.n)}, device_id_type=MESH)
        return 0
    lax.fori_loop(1, d.n, greet, 0)

    def exchange(e, snd, rcv):
        return Exchange(d, me, tor, snd, rcv, esem.at[e])

    ex = [[exchange(i * d.nc + c, send.at[i, c], recv.at[i, c])
           for c in range(d.nc)] for i in range(4)]
    ships = [[exchange((4 + i) * d.nc + c, ship.at[i, c], shipr.at[i, c]) for c in range(d.nc)] for i in range(2)]

    def dispatch(i, c, st):
        def fill(s):
            send[i, c, s] = st[message_rows(d, s), :].astype(BF16)
        loop(d.n, fill, 4)
        ex[i][c].start()

    def collect(i, c, st):
        ex[i][c].collect()

        def take(s):
            st[message_rows(d, s), :] = recv[i, c, s].astype(F32)
        loop(d.n, take, 4)

    for c in range(d.nc):
        loads[c].wait()
        if c == 0:
            tables.wait()
            for x in small + wloads + [gload]:
                x.start()

        def analysis_step(p):
            bt = c * d.bt + 2 * p
            y = analyse(jnp.concatenate([f[bt], f[bt + 1]], axis=1), ah, al)
            for u, half in enumerate(lane_halves(d)):
                put_modes(d, stage, y, 2 * p + u, half)
        loop(d.bt // 2, analysis_step, 3)
        if c == 0:
            pl.semaphore_wait(bar, d.n - 1)
        dispatch(0, c, stage)
    for x in small:
        x.wait()
    permuted(d, perm, pf, pw, pwt)
    permuted(d, perm, pi, pv, pvt)
    for j in range(d.t):
        wloads[j].wait()

        def prepare(ll):
            for r in range(2):
                w[d.n * j + ll, r * d.c:(r + 1) * d.c, :] = full[j, ll, pl.ds(r, d.c, stride=2), :].astype(BF16)
        loop(d.n, prepare, 4)

    for c in range(d.nc):
        collect(0, c, stage2)
        to_spectral(d, stage2, spec, turn, pw, 1.0)
        extract(d, spec, ship.at[0, c])
        mix(d, spec, turn, spec2, w, True)
        from_spectral(d, spec2, stage, pvt)
        dispatch(1, c, stage)
    for c in range(d.nc):
        ships[0][c].start()
    gload.wait()
    for c in range(d.nc):
        collect(1, c, stage2)

        def grid_step(p):
            bt = 2 * p
            at = c * d.bt + bt
            g = jnp.concatenate([get_modes(d, stage2, bt), get_modes(d, stage2, bt + 1)], axis=1).astype(BF16)
            h = mm(sh[...], g) + mm(sl[...], g)
            u = jnp.concatenate([dg[at], dg[at + 1]], axis=1) * gelu_grad(h)
            y = analyse(u, bh, bl)
            for i, half in enumerate(lane_halves(d)):
                put_modes(d, stage, y, bt + i, half)
        loop(d.bt // 2, grid_step, 2)
        dispatch(2, c, stage)
    for c in range(d.nc):
        collect(2, c, stage2)
        to_spectral(d, stage2, spec, turn, pv, -1.0)
        extract(d, spec, ship.at[1, c])
        ships[1][c].start()
        mix(d, spec, turn, spec2, w, False)
        from_spectral(d, spec2, stage, pwt)
        dispatch(3, c, stage)
        if c + 1 == d.nc:
            for e in ships[0] + ships[1][:c]:
                e.collect()
    for c in range(d.nc):
        if c + 1 == d.nc:
            ships[1][c].collect()
        for j, y in enumerate(weights(d, shipr.at[0, c], shipr.at[1, c])):
            if c + 1 < d.nc:
                wsum[j] = y if c == 0 else wsum[j] + y
            else:
                y = wsum[j] + y
                for r, half in enumerate(lane_halves(d)):
                    full[j, me, pl.ds(r, d.c, stride=2), :] = y[:, half]
    gather = Gather(d, me, tor, full, gsem.at[0], r1, r2, rp)

    def finish(c):
        def task():
            collect(3, c, stage2)

            def step(p):
                bt = 2 * p
                at = c * d.bt + bt
                g = jnp.concatenate([get_modes(d, stage2, bt), get_modes(d, stage2, bt + 1)], axis=1).astype(BF16)
                y = mm(zh[...], g) + mm(zl[...], g)
                for i, half in enumerate(lane_halves(d)):
                    df[at + i] = dg[at + i] + y[:, half]
            loop(d.bt // 2, step, 2)
        return task
    gather.run([finish(c) for c in range(d.nc)])
    for e in sum(ex + ships, []):
        e.drain()


def final_kernel(df, full, out, dw, sem):
    copies = [pltpu.make_async_copy(full.at[j], dw.at[j], sem.at[j]) for j in range(full.shape[0])]
    copies.append(pltpu.make_async_copy(df, out, sem.at[full.shape[0]]))
    for c in copies:
        c.start()
    for c in copies:
        c.wait()


def solution(mesh):
    n = mesh.shape['lat']
    field_spec = P('member', None, 'lat', None)

    def local_step(field_loc, grad_loc, p_fwd, p_inv, w_mix):
        batch, chan, rows, lon = field_loc.shape
        d = Dims(n, batch, chan, rows, lon)
        tables = np.stack([m for pair in dft_constants(d) for m in pair])
        perm = perm_constant(d)
        f = field_loc.transpose(0, 2, 3, 1).reshape(batch * rows, lon, chan)
        dg = grad_loc.transpose(0, 2, 3, 1).reshape(batch * rows, lon, chan)
        w = w_mix.transpose(0, 1, 3, 2).reshape(rows, n, 2 * chan, chan)

        nc = d.nc
        shipped = VMEM((2, nc, n, d.ship_off[-1], chan), BF16)
        message = VMEM((4, nc, n, d.msg, chan), BF16)
        stage = VMEM((n * d.msg, chan), F32)
        spec = VMEM((2 * rows * d.b * d.lp, chan), F32)
        mat = VMEM((rows, d.lat, d.lat), BF16)
        raw = VMEM((rows, d.lat, d.lat), F32)
        field = VMEM(f.shape, F32)
        dma = lambda *s: pltpu.SemaphoreType.DMA(s)
        vspec = pl.BlockSpec(memory_space=VMEM)
        hspec = pl.BlockSpec(memory_space=pltpu.HBM)
        df, full = pl.pallas_call(
            functools.partial(main_kernel, d), name="main",
            out_shape=[VMEM(f.shape, F32), VMEM(w.shape, F32)],
            in_specs=[hspec] * 7,
            out_specs=[vspec, vspec],
            scratch_shapes=[VMEM(perm.shape, BF16), VMEM(tables.shape, BF16), VMEM((rows, chan, 2 * chan), F32), field, field,
                            VMEM((d.lat, 2 * chan, chan), BF16), raw, raw, mat, mat, mat, mat, stage, stage, spec, spec, spec,
                            message, message, shipped, shipped,
                            dma(nc + 9 + rows), dma(6 * nc, 2), dma(1), dma(4), dma(4, 4), dma(16)],
            compiler_params=pltpu.CompilerParams(collective_id=0, has_side_effects=True, vmem_limit_bytes=49 * 1024 * 1024),
        )(f, dg, w, p_fwd, p_inv, perm, tables)
        df, dw = pl.pallas_call(
            final_kernel, name="final",
            out_shape=[jax.ShapeDtypeStruct(f.shape, F32), jax.ShapeDtypeStruct(w.shape, F32)],
            in_specs=[vspec, vspec], out_specs=[hspec, hspec],
            scratch_shapes=[dma(rows + 1)],
            compiler_params=pltpu.CompilerParams(vmem_limit_bytes=1024 * 1024),
        )(df, full)
        grad_field = df.reshape(batch, rows, lon, chan).transpose(0, 3, 1, 2)
        grad_wmix = dw.reshape(d.lat, chan, 2, chan).transpose(0, 1, 3, 2)
        return grad_field, grad_wmix

    return jax.shard_map(local_step, mesh=mesh, in_specs=(field_spec, field_spec, P(), P(), P()), out_specs=(field_spec, P('member', None, None, None)), check_vma=False)
```

```python
import functools
import math
import random
import numpy as np
import jax
import jax.numpy as jnp
from jax import lax
from jax.experimental import pallas as pl
from jax.experimental.pallas import tpu as pltpu
from jax.sharding import PartitionSpec as P

MESH = pl.DeviceIdType.MESH
F32, BF16 = jnp.float32, jnp.bfloat16
VMEM = pltpu.VMEM


class Dims:
    def __init__(self, n, batch, chan, rows, lon):
        self.n = n
        self.side = math.isqrt(n // 2)
        self.seed = 0
        self.nc = 2
        self.b, self.c, self.t, self.lon = batch // self.nc, chan, rows, lon
        self.lat = n * rows
        self.bt = self.b * rows
        self.msg = 2 * rows * self.bt
        self.lp = self.lat + 8
        self.ship_off = [self.b * j * (j + 1) for j in range(rows + 1)]


def split_const(mat):
    hi = mat.astype(jnp.bfloat16)
    lo = (mat - hi.astype(np.float64)).astype(jnp.bfloat16)
    return hi, lo


def dft_constants(d):
    m = np.arange(d.lat)
    ang = 2.0 * np.pi * np.outer(m, np.arange(d.lon)) / d.lon
    scale = 1.0 / math.sqrt(d.lon)
    ana = scale * np.concatenate([np.cos(ang), -np.sin(ang)])
    gain = np.where(m == 0, 1.0, 2.0)[:, None]
    ana2 = scale * np.concatenate([np.cos(ang) * gain, -np.sin(ang) * gain])
    syn = ana2.T
    syn2 = ana.T
    return [split_const(a) for a in (ana, ana2, syn, syn2)]


def perm_constant(d):
    t = np.arange(d.lat)
    tau = (t % d.t) * d.n + t // d.t
    mat = np.zeros((d.lat, d.lat))
    mat[t, tau] = 1.0
    return mat.astype(jnp.bfloat16)


def mm(a, b):
    return jnp.dot(a, b, preferred_element_type=F32)


def mm_nt(a, b):
    return lax.dot_general(a, b, (((1,), (1,)), ((), ())), preferred_element_type=F32)


def mm_tn(a, b):
    return lax.dot_general(a, b, (((0,), (0,)), ((), ())), preferred_element_type=F32)


def rnd(x):
    return x.astype(BF16).astype(F32)


class Torus:
    def __init__(self, d, me):
        side = d.side
        y, x, h = me // (2 * side), lax.rem(me // 2, side), lax.rem(me, 2)
        self.side, self.h = side, h
        way = 1 - 2 * h
        self.ys = [lax.rem(y + way * i + side, side) * (2 * side) for i in range(side)]
        self.xs = [lax.rem(x + way * i + side, side) * 2 for i in range(side)]
        self.hs = [h, 1 - h]

    def at(self, dy, dx, dh):
        return self.ys[dy % self.side] + self.xs[dx % self.side] + self.hs[dh % 2]


def remote(src, dst, ssem, rsem, to):
    return pltpu.make_async_remote_copy(src_ref=src, dst_ref=dst, send_sem=ssem, recv_sem=rsem,
                                        device_id={"lat": to}, device_id_type=MESH)


class Exchange:
    def __init__(self, d, me, tor, send, recv, sems):
        self.d, self.me, self.tor, self.send, self.recv = d, me, tor, send, recv
        self.ssem, self.rsem = sems.at[0], sems.at[1]
        self.offsets = [(dy, dx, dh) for dy in range(d.side) for dx in range(d.side) for dh in range(2)][1:]
        random.Random(d.seed).shuffle(self.offsets)

    def start(self):
        for o in self.offsets:
            to = self.tor.at(*o)
            remote(self.send.at[to], self.recv.at[self.me], self.ssem, self.rsem, to).start()

    def wait(self, ref, sem):
        pltpu.make_async_copy(ref, ref, sem).wait()

    def collect(self):
        self.recv[self.me] = self.send[self.me]
        self.wait(self.recv.at[0:self.d.n - 1], self.rsem)

    def drain(self):
        self.wait(self.send.at[0:self.d.n - 1], self.ssem)


def message_rows(d, s):
    return pl.ds(pl.multiple_of(s * d.msg, 8), d.msg)


def ring_rows(d, start):
    return pl.ds(start, d.n, stride=d.msg)


def put_modes(d, stage, y, bt, lanes):
    for rk in range(2 * d.t):
        stage[ring_rows(d, rk * d.bt + bt), :] = y[rk * d.n:(rk + 1) * d.n, lanes]


def get_modes(d, stage, bt):
    return jnp.concatenate([stage[ring_rows(d, rk * d.bt + bt), :] for rk in range(2 * d.t)], axis=0)


def analyse(x, hi, lo):
    xh = x.astype(BF16)
    xl = (x - xh.astype(F32)).astype(BF16)
    return mm(hi[...], xh) + mm(lo[...], xh) + mm(hi[...], xl)


def loop(count, body, unroll=1):
    def step(i, _):
        body(i)
        return 0
    lax.fori_loop(0, count, step, 0, unroll=unroll)


def lane_halves(d):
    return slice(0, d.c), slice(d.c, 2 * d.c)


def permuted(d, perm, p, out, outt):
    for k in range(d.t):
        pk = p[k].astype(BF16)
        out[k] = mm(pk, perm[...]).astype(BF16)
        outt[k] = mm_tn(perm[...], pk.T).astype(BF16)


def spec_at(d, r, k, b):
    return pl.multiple_of(((k * 2 + r) * d.b + b) * d.lp + d.n * k, 8)


def to_spectral(d, stage, spec, turn, p, sign):
    for k in range(d.t):
        low = d.n * k

        def body(b):
            x = jnp.concatenate([jnp.concatenate(
                [stage[ring_rows(d, (r * d.t + k) * d.bt + b * d.t + t), :] for t in range(d.t)], axis=0)
                for r in range(2)], axis=1)
            y = rnd(mm(p[k, low:, :], x.astype(BF16)))
            for r, half in enumerate(lane_halves(d)):
                spec[pl.ds(spec_at(d, r, k, b), d.lat - low), :] = y[:, half]
                turn[pl.ds(spec_at(d, 1 - r, k, b), d.lat - low), :] = y[:, half] * (sign if r == 0 else -sign)
        loop(d.b, body, d.b)


def from_spectral(d, spec, stage, pt):
    for k in range(d.t):
        low = d.n * k

        def body(b):
            x = jnp.concatenate([spec[pl.ds(spec_at(d, r, k, b), d.lat - low), :] for r in range(2)], axis=1).astype(BF16)
            y = mm(pt[k][:, low:], x)
            for r, half in enumerate(lane_halves(d)):
                for t in range(d.t):
                    stage[ring_rows(d, (r * d.t + k) * d.bt + b * d.t + t), :] = y[t * d.n:(t + 1) * d.n, half]
        loop(d.b, body, d.b)


def extract(d, spec, ship):
    for j in range(d.t):
        def body(ll):
            ship[ll, d.ship_off[j]:d.ship_off[j + 1], :] = spec[pl.ds(d.n * j + ll, 2 * d.b * (j + 1), stride=d.lp), :].astype(BF16)
        loop(d.n, body, 8)


def mix(d, spec, turn, out, w, forward):
    for j in range(d.t):
        rows = 2 * d.b * (j + 1)

        def body(ll):
            l = d.n * j + ll
            at = pl.ds(l, rows, stride=d.lp)
            x = spec[at, :].astype(BF16)
            x2 = jnp.concatenate([x, turn[at, :].astype(BF16)], axis=1)
            if forward:
                y = mm_nt(x2, jnp.concatenate([w[l, :d.c, :], w[l, d.c:, :]], axis=1))
            else:
                y = mm(x2, w[l])
            out[at, :] = rnd(y)
        loop(d.n, body, 8)


def gelu_grad(values):
    cumulative = 0.5 * (1.0 + lax.erf(values * math.sqrt(0.5)))
    density = jnp.exp(-0.5 * values * values) * (1.0 / math.sqrt(2.0 * math.pi))
    return cumulative + values * density


def weights(d, a, dq):
    parts = []
    for j in range(d.t):
        at = slice(d.ship_off[j], d.ship_off[j + 1])
        groups = d.n * (j + 1)
        x = a[:, at, :].astype(F32).reshape(groups, 2 * d.b, d.c)
        turn = jnp.concatenate([-x[:, d.b:, :], x[:, :d.b, :]], axis=1)
        both = jnp.concatenate([x, turn], axis=2).reshape(groups * 2 * d.b, 2 * d.c)
        g = dq[:, at, :].astype(F32).reshape(groups * 2 * d.b, d.c)
        parts.append(mm_tn(g.astype(BF16), both.astype(BF16)))
    return parts


class Gather:
    def __init__(self, d, me, tor, full, ssem, r1, r2, rp):
        self.d, self.me, self.tor, self.full = d, me, tor, full
        self.ssem, self.r1, self.r2, self.rp = ssem, r1, r2, rp
        self.half = full.shape[2] // 2
        h, side = tor.h, tor.side
        self.first = [lax.select(h == 0, tor.xs[i], tor.ys[i]) for i in range(side)]
        self.second = [lax.select(h == 0, tor.ys[i], tor.xs[i]) for i in range(side)]

    def near(self, one, two):
        return self.first[one % self.d.side] + self.second[two % self.d.side] + self.tor.h

    def piece(self, block, part):
        if part is None:
            return self.full.at[:, block]
        return self.full.at[:, block, self.half * part:self.half * (part + 1), :]

    def start(self, block, part, rsem, to):
        ref = self.piece(block, part)
        remote(ref, ref, self.ssem, rsem, to).start()

    def arrive(self, block, part, rsem):
        ref = self.piece(block, part)
        pltpu.make_async_copy(ref, ref, rsem).wait()

    def run(self, tasks):
        near, r1, r2, rp = self.near, self.r1, self.r2, self.rp
        partner = self.tor.at(0, 0, 1)
        pos = [0, -1, 1, 2]
        p1, m1, p2, m2 = near(1, 0), near(-1, 0), near(0, 1), near(0, -1)
        group = [near(i, 0) for i in pos]

        def second(q):
            self.start(group[q], None, r2.at[q, 0], p2)
            self.start(group[q], None, r2.at[q, 1], m2)
            self.start(group[q], None, rp.at[q], partner)

        def relay(q):
            for i, (off, to) in enumerate(((-1, p2), (1, m2))):
                block = near(pos[q], off)
                self.arrive(block, None, r2.at[q, i])
                self.start(block, i, r2.at[q, 2 + i], to)
                self.start(block, None, rp.at[4 + 2 * q + i], partner)

        self.start(group[0], None, r1.at[0], p1)
        self.start(group[0], None, r1.at[1], m1)
        second(0)
        tasks[0]()
        self.arrive(group[1], None, r1.at[0])
        self.start(group[1], 0, r1.at[2], p1)
        second(1)
        self.arrive(group[2], None, r1.at[1])
        self.start(group[2], 1, r1.at[3], m1)
        second(2)
        tasks[1]()
        relay(0)
        self.arrive(group[3], 0, r1.at[2])
        self.arrive(group[3], 1, r1.at[3])
        second(3)
        for q in (1, 2, 3):
            relay(q)
        for q in range(4):
            block = near(pos[q], 2)
            for i in range(2):
                self.arrive(block, i, r2.at[q, 2 + i])
            self.start(block, None, rp.at[12 + q], partner)
        for i in range(16):
            self.arrive(partner, None, rp.at[i])
        every = self.full.at[:, 0:31]
        pltpu.make_async_copy(every, every, self.ssem).wait()


def main_kernel(d, f_h, dg_h, w_h, pf_h, pi_h, perm_h, dft_h, df, full,
                perm, dft, wsum, f, dg, w, pf, pi, pw, pwt, pv, pvt, stage, stage2, spec, turn, spec2, send, recv, ship, shipr,
                isem, esem, gsem, r1, r2, rp):
    me = lax.axis_index("lat")
    tor = Torus(d, me)
    bar = pltpu.get_barrier_semaphore()
    loads = [pltpu.make_async_copy(f_h.at[c * d.bt:(c + 1) * d.bt], f.at[c * d.bt:(c + 1) * d.bt], isem.at[c]) for c in range(d.nc)]
    ah, al, bh, bl, sh, sl, zh, zl = [dft.at[i] for i in range(8)]
    tables = pltpu.make_async_copy(dft_h, dft, isem.at[d.nc + 7 + d.t])
    small = [pltpu.make_async_copy(perm_h, perm, isem.at[d.nc + 8 + d.t])]
    for k in range(d.t):
        small.append(pltpu.make_async_copy(pf_h.at[me + k * d.n], pf.at[k], isem.at[d.nc + 2 * k]))
        small.append(pltpu.make_async_copy(pi_h.at[me + k * d.n], pi.at[k], isem.at[d.nc + 2 * k + 1]))
    wloads = [pltpu.make_async_copy(w_h.at[j], full.at[j], isem.at[d.nc + 6 + j]) for j in range(d.t)]
    gload = pltpu.make_async_copy(dg_h, dg, isem.at[d.nc + 6 + d.t])
    for c in loads[:1] + [tables] + loads[1:]:
        c.start()

    def greet(k, _):
        pl.semaphore_signal(bar, inc=1, device_id={"lat": lax.rem(me + k, d.n)}, device_id_type=MESH)
        return 0
    lax.fori_loop(1, d.n, greet, 0)

    def exchange(e, snd, rcv):
        return Exchange(d, me, tor, snd, rcv, esem.at[e])

    ex = [[exchange(i * d.nc + c, send.at[i, c], recv.at[i, c])
           for c in range(d.nc)] for i in range(4)]
    ships = [[exchange((4 + i) * d.nc + c, ship.at[i, c], shipr.at[i, c]) for c in range(d.nc)] for i in range(2)]

    def dispatch(i, c, st):
        def fill(s):
            send[i, c, s] = st[message_rows(d, s), :].astype(BF16)
        loop(d.n, fill, 4)
        ex[i][c].start()

    def collect(i, c, st):
        ex[i][c].collect()

        def take(s):
            st[message_rows(d, s), :] = recv[i, c, s].astype(F32)
        loop(d.n, take, 4)

    for c in range(d.nc):
        loads[c].wait()
        if c == 0:
            tables.wait()
            for x in small + wloads + [gload]:
                x.start()

        def analysis_step(p):
            bt = c * d.bt + 2 * p
            y = analyse(jnp.concatenate([f[bt], f[bt + 1]], axis=1), ah, al)
            for u, half in enumerate(lane_halves(d)):
                put_modes(d, stage, y, 2 * p + u, half)
        loop(d.bt // 2, analysis_step, 3)
        if c == 0:
            pl.semaphore_wait(bar, d.n - 1)
        dispatch(0, c, stage)
    for x in small:
        x.wait()
    permuted(d, perm, pf, pw, pwt)
    permuted(d, perm, pi, pv, pvt)
    for j in range(d.t):
        wloads[j].wait()

        def prepare(ll):
            for r in range(2):
                w[d.n * j + ll, r * d.c:(r + 1) * d.c, :] = full[j, ll, pl.ds(r, d.c, stride=2), :].astype(BF16)
        loop(d.n, prepare, 4)

    for c in range(d.nc):
        collect(0, c, stage2)
        to_spectral(d, stage2, spec, turn, pw, 1.0)
        extract(d, spec, ship.at[0, c])
        mix(d, spec, turn, spec2, w, True)
        from_spectral(d, spec2, stage, pvt)
        dispatch(1, c, stage)
    for c in range(d.nc):
        ships[0][c].start()
    gload.wait()
    for c in range(d.nc):
        collect(1, c, stage2)

        def grid_step(p):
            bt = 2 * p
            at = c * d.bt + bt
            g = jnp.concatenate([get_modes(d, stage2, bt), get_modes(d, stage2, bt + 1)], axis=1).astype(BF16)
            h = mm(sh[...], g) + mm(sl[...], g)
            u = jnp.concatenate([dg[at], dg[at + 1]], axis=1) * gelu_grad(h)
            y = analyse(u, bh, bl)
            for i, half in enumerate(lane_halves(d)):
                put_modes(d, stage, y, bt + i, half)
        loop(d.bt // 2, grid_step, 2)
        dispatch(2, c, stage)
    for c in range(d.nc):
        collect(2, c, stage2)
        to_spectral(d, stage2, spec, turn, pv, -1.0)
        extract(d, spec, ship.at[1, c])
        ships[1][c].start()
        mix(d, spec, turn, spec2, w, False)
        from_spectral(d, spec2, stage, pwt)
        dispatch(3, c, stage)
        if c + 1 == d.nc:
            for e in ships[0] + ships[1][:c]:
                e.collect()
    for c in range(d.nc):
        if c + 1 == d.nc:
            ships[1][c].collect()
        for j, y in enumerate(weights(d, shipr.at[0, c], shipr.at[1, c])):
            if c + 1 < d.nc:
                wsum[j] = y if c == 0 else wsum[j] + y
            else:
                y = wsum[j] + y
                for r, half in enumerate(lane_halves(d)):
                    full[j, me, pl.ds(r, d.c, stride=2), :] = y[:, half]
    gather = Gather(d, me, tor, full, gsem.at[0], r1, r2, rp)

    def finish(c):
        def task():
            collect(3, c, stage2)

            def step(p):
                bt = 2 * p
                at = c * d.bt + bt
                g = jnp.concatenate([get_modes(d, stage2, bt), get_modes(d, stage2, bt + 1)], axis=1).astype(BF16)
                y = mm(zh[...], g) + mm(zl[...], g)
                for i, half in enumerate(lane_halves(d)):
                    df[at + i] = dg[at + i] + y[:, half]
            loop(d.bt // 2, step, 2)
        return task
    gather.run([finish(c) for c in range(d.nc)])
    for e in sum(ex + ships, []):
        e.drain()


def final_kernel(df, full, out, dw, sem):
    copies = [pltpu.make_async_copy(full.at[j], dw.at[j], sem.at[j]) for j in range(full.shape[0])]
    copies.append(pltpu.make_async_copy(df, out, sem.at[full.shape[0]]))
    for c in copies:
        c.start()
    for c in copies:
        c.wait()


def solution(mesh):
    n = mesh.shape['lat']
    field_spec = P('member', None, 'lat', None)

    def local_step(field_loc, grad_loc, p_fwd, p_inv, w_mix):
        batch, chan, rows, lon = field_loc.shape
        d = Dims(n, batch, chan, rows, lon)
        tables = np.stack([m for pair in dft_constants(d) for m in pair])
        perm = perm_constant(d)
        f = field_loc.transpose(0, 2, 3, 1).reshape(batch * rows, lon, chan)
        dg = grad_loc.transpose(0, 2, 3, 1).reshape(batch * rows, lon, chan)
        w = w_mix.transpose(0, 1, 3, 2).reshape(rows, n, 2 * chan, chan)

        nc = d.nc
        shipped = VMEM((2, nc, n, d.ship_off[-1], chan), BF16)
        message = VMEM((4, nc, n, d.msg, chan), BF16)
        stage = VMEM((n * d.msg, chan), F32)
        spec = VMEM((2 * rows * d.b * d.lp, chan), F32)
        mat = VMEM((rows, d.lat, d.lat), BF16)
        raw = VMEM((rows, d.lat, d.lat), F32)
        field = VMEM(f.shape, F32)
        dma = lambda *s: pltpu.SemaphoreType.DMA(s)
        vspec = pl.BlockSpec(memory_space=VMEM)
        hspec = pl.BlockSpec(memory_space=pltpu.HBM)
        df, full = pl.pallas_call(
            functools.partial(main_kernel, d), name="main",
            out_shape=[VMEM(f.shape, F32), VMEM(w.shape, F32)],
            in_specs=[hspec] * 7,
            out_specs=[vspec, vspec],
            scratch_shapes=[VMEM(perm.shape, BF16), VMEM(tables.shape, BF16), VMEM((rows, chan, 2 * chan), F32), field, field,
                            VMEM((d.lat, 2 * chan, chan), BF16), raw, raw, mat, mat, mat, mat, stage, stage, spec, spec, spec,
                            message, message, shipped, shipped,
                            dma(nc + 9 + rows), dma(6 * nc, 2), dma(1), dma(4), dma(4, 4), dma(16)],
            compiler_params=pltpu.CompilerParams(collective_id=0, has_side_effects=True, vmem_limit_bytes=49 * 1024 * 1024),
        )(f, dg, w, p_fwd, p_inv, perm, tables)
        df, dw = pl.pallas_call(
            final_kernel, name="final",
            out_shape=[jax.ShapeDtypeStruct(f.shape, F32), jax.ShapeDtypeStruct(w.shape, F32)],
            in_specs=[vspec, vspec], out_specs=[hspec, hspec],
            scratch_shapes=[dma(rows + 1)],
            compiler_params=pltpu.CompilerParams(vmem_limit_bytes=1024 * 1024),
        )(df, full)
        grad_field = df.reshape(batch, rows, lon, chan).transpose(0, 3, 1, 2)
        grad_wmix = dw.reshape(d.lat, chan, 2, chan).transpose(0, 1, 3, 2)
        return grad_field, grad_wmix

    return jax.shard_map(local_step, mesh=mesh, in_specs=(field_spec, field_spec, P(), P(), P()), out_specs=(field_spec, P('member', None, None, None)), check_vma=False)
```

```python
import functools
import math
import random
import numpy as np
import jax
import jax.numpy as jnp
from jax import lax
from jax.experimental import pallas as pl
from jax.experimental.pallas import tpu as pltpu
from jax.sharding import PartitionSpec as P

MESH = pl.DeviceIdType.MESH
F32, BF16 = jnp.float32, jnp.bfloat16
VMEM = pltpu.VMEM


class Dims:
    def __init__(self, n, batch, chan, rows, lon):
        self.n = n
        self.side = math.isqrt(n // 2)
        self.seed = 4
        self.nc = 2
        self.b, self.c, self.t, self.lon = batch // self.nc, chan, rows, lon
        self.lat = n * rows
        self.bt = self.b * rows
        self.msg = 2 * rows * self.bt
        self.lp = self.lat + 8
        self.ship_off = [self.b * j * (j + 1) for j in range(rows + 1)]


def split_const(mat):
    hi = mat.astype(jnp.bfloat16)
    lo = (mat - hi.astype(np.float64)).astype(jnp.bfloat16)
    return hi, lo


def dft_constants(d):
    m = np.arange(d.lat)
    ang = 2.0 * np.pi * np.outer(m, np.arange(d.lon)) / d.lon
    scale = 1.0 / math.sqrt(d.lon)
    ana = scale * np.concatenate([np.cos(ang), -np.sin(ang)])
    gain = np.where(m == 0, 1.0, 2.0)[:, None]
    ana2 = scale * np.concatenate([np.cos(ang) * gain, -np.sin(ang) * gain])
    syn = ana2.T
    syn2 = ana.T
    return [split_const(a) for a in (ana, ana2, syn, syn2)]


def perm_constant(d):
    t = np.arange(d.lat)
    tau = (t % d.t) * d.n + t // d.t
    mat = np.zeros((d.lat, d.lat))
    mat[t, tau] = 1.0
    return mat.astype(jnp.bfloat16)


def mm(a, b):
    return jnp.dot(a, b, preferred_element_type=F32)


def mm_nt(a, b):
    return lax.dot_general(a, b, (((1,), (1,)), ((), ())), preferred_element_type=F32)


def mm_tn(a, b):
    return lax.dot_general(a, b, (((0,), (0,)), ((), ())), preferred_element_type=F32)


def rnd(x):
    return x.astype(BF16).astype(F32)


class Torus:
    def __init__(self, d, me):
        side = d.side
        y, x, h = me // (2 * side), lax.rem(me // 2, side), lax.rem(me, 2)
        self.side, self.h = side, h
        way = 1 - 2 * h
        self.ys = [lax.rem(y + way * i + side, side) * (2 * side) for i in range(side)]
        self.xs = [lax.rem(x + way * i + side, side) * 2 for i in range(side)]
        self.hs = [h, 1 - h]

    def at(self, dy, dx, dh):
        return self.ys[dy % self.side] + self.xs[dx % self.side] + self.hs[dh % 2]


def remote(src, dst, ssem, rsem, to):
    return pltpu.make_async_remote_copy(src_ref=src, dst_ref=dst, send_sem=ssem, recv_sem=rsem,
                                        device_id={"lat": to}, device_id_type=MESH)


class Exchange:
    def __init__(self, d, me, tor, send, recv, sems):
        self.d, self.me, self.tor, self.send, self.recv = d, me, tor, send, recv
        self.ssem, self.rsem = sems.at[0], sems.at[1]
        self.offsets = [(dy, dx, dh) for dy in range(d.side) for dx in range(d.side) for dh in range(2)][1:]
        random.Random(d.seed).shuffle(self.offsets)

    def start(self):
        for o in self.offsets:
            to = self.tor.at(*o)
            remote(self.send.at[to], self.recv.at[self.me], self.ssem, self.rsem, to).start()

    def wait(self, ref, sem):
        pltpu.make_async_copy(ref, ref, sem).wait()

    def collect(self):
        self.recv[self.me] = self.send[self.me]
        self.wait(self.recv.at[0:self.d.n - 1], self.rsem)

    def drain(self):
        self.wait(self.send.at[0:self.d.n - 1], self.ssem)


def message_rows(d, s):
    return pl.ds(pl.multiple_of(s * d.msg, 8), d.msg)


def ring_rows(d, start):
    return pl.ds(start, d.n, stride=d.msg)


def put_modes(d, stage, y, bt, lanes):
    for rk in range(2 * d.t):
        stage[ring_rows(d, rk * d.bt + bt), :] = y[rk * d.n:(rk + 1) * d.n, lanes]


def get_modes(d, stage, bt):
    return jnp.concatenate([stage[ring_rows(d, rk * d.bt + bt), :] for rk in range(2 * d.t)], axis=0)


def analyse(x, hi, lo):
    xh = x.astype(BF16)
    xl = (x - xh.astype(F32)).astype(BF16)
    return mm(hi[...], xh) + mm(lo[...], xh) + mm(hi[...], xl)


def loop(count, body, unroll=1):
    def step(i, _):
        body(i)
        return 0
    lax.fori_loop(0, count, step, 0, unroll=unroll)


def lane_halves(d):
    return slice(0, d.c), slice(d.c, 2 * d.c)


def permuted(d, perm, p, out, outt):
    for k in range(d.t):
        pk = p[k].astype(BF16)
        out[k] = mm(pk, perm[...]).astype(BF16)
        outt[k] = mm_tn(perm[...], pk.T).astype(BF16)


def spec_at(d, r, k, b):
    return pl.multiple_of(((k * 2 + r) * d.b + b) * d.lp + d.n * k, 8)


def to_spectral(d, stage, spec, turn, p, sign):
    for k in range(d.t):
        low = d.n * k

        def body(b):
            x = jnp.concatenate([jnp.concatenate(
                [stage[ring_rows(d, (r * d.t + k) * d.bt + b * d.t + t), :] for t in range(d.t)], axis=0)
                for r in range(2)], axis=1)
            y = rnd(mm(p[k, low:, :], x.astype(BF16)))
            for r, half in enumerate(lane_halves(d)):
                spec[pl.ds(spec_at(d, r, k, b), d.lat - low), :] = y[:, half]
                turn[pl.ds(spec_at(d, 1 - r, k, b), d.lat - low), :] = y[:, half] * (sign if r == 0 else -sign)
        loop(d.b, body, d.b)


def from_spectral(d, spec, stage, pt):
    for k in range(d.t):
        low = d.n * k

        def body(b):
            x = jnp.concatenate([spec[pl.ds(spec_at(d, r, k, b), d.lat - low), :] for r in range(2)], axis=1).astype(BF16)
            y = mm(pt[k][:, low:], x)
            for r, half in enumerate(lane_halves(d)):
                for t in range(d.t):
                    stage[ring_rows(d, (r * d.t + k) * d.bt + b * d.t + t), :] = y[t * d.n:(t + 1) * d.n, half]
        loop(d.b, body, d.b)


def extract(d, spec, ship):
    for j in range(d.t):
        def body(ll):
            ship[ll, d.ship_off[j]:d.ship_off[j + 1], :] = spec[pl.ds(d.n * j + ll, 2 * d.b * (j + 1), stride=d.lp), :].astype(BF16)
        loop(d.n, body, 8)


def mix(d, spec, turn, out, w, forward):
    for j in range(d.t):
        rows = 2 * d.b * (j + 1)

        def body(ll):
            l = d.n * j + ll
            at = pl.ds(l, rows, stride=d.lp)
            x = spec[at, :].astype(BF16)
            x2 = jnp.concatenate([x, turn[at, :].astype(BF16)], axis=1)
            if forward:
                y = mm_nt(x2, jnp.concatenate([w[l, :d.c, :], w[l, d.c:, :]], axis=1))
            else:
                y = mm(x2, w[l])
            out[at, :] = rnd(y)
        loop(d.n, body, 8)


def gelu_grad(values):
    cumulative = 0.5 * (1.0 + lax.erf(values * math.sqrt(0.5)))
    density = jnp.exp(-0.5 * values * values) * (1.0 / math.sqrt(2.0 * math.pi))
    return cumulative + values * density


def weights(d, a, dq):
    parts = []
    for j in range(d.t):
        at = slice(d.ship_off[j], d.ship_off[j + 1])
        groups = d.n * (j + 1)
        x = a[:, at, :].astype(F32).reshape(groups, 2 * d.b, d.c)
        turn = jnp.concatenate([-x[:, d.b:, :], x[:, :d.b, :]], axis=1)
        both = jnp.concatenate([x, turn], axis=2).reshape(groups * 2 * d.b, 2 * d.c)
        g = dq[:, at, :].astype(F32).reshape(groups * 2 * d.b, d.c)
        parts.append(mm_tn(g.astype(BF16), both.astype(BF16)))
    return parts


class Gather:
    def __init__(self, d, me, tor, full, ssem, r1, r2, rp):
        self.d, self.me, self.tor, self.full = d, me, tor, full
        self.ssem, self.r1, self.r2, self.rp = ssem, r1, r2, rp
        self.half = full.shape[2] // 2
        h, side = tor.h, tor.side
        self.first = [lax.select(h == 0, tor.xs[i], tor.ys[i]) for i in range(side)]
        self.second = [lax.select(h == 0, tor.ys[i], tor.xs[i]) for i in range(side)]

    def near(self, one, two):
        return self.first[one % self.d.side] + self.second[two % self.d.side] + self.tor.h

    def piece(self, block, part):
        if part is None:
            return self.full.at[:, block]
        return self.full.at[:, block, self.half * part:self.half * (part + 1), :]

    def start(self, block, part, rsem, to):
        ref = self.piece(block, part)
        remote(ref, ref, self.ssem, rsem, to).start()

    def arrive(self, block, part, rsem):
        ref = self.piece(block, part)
        pltpu.make_async_copy(ref, ref, rsem).wait()

    def run(self, tasks):
        near, r1, r2, rp = self.near, self.r1, self.r2, self.rp
        partner = self.tor.at(0, 0, 1)
        pos = [0, -1, 1, 2]
        p1, m1, p2, m2 = near(1, 0), near(-1, 0), near(0, 1), near(0, -1)
        group = [near(i, 0) for i in pos]

        def second(q):
            self.start(group[q], None, r2.at[q, 0], p2)
            self.start(group[q], None, r2.at[q, 1], m2)
            self.start(group[q], None, rp.at[q], partner)

        def relay(q):
            for i, (off, to) in enumerate(((-1, p2), (1, m2))):
                block = near(pos[q], off)
                self.arrive(block, None, r2.at[q, i])
                self.start(block, i, r2.at[q, 2 + i], to)
                self.start(block, None, rp.at[4 + 2 * q + i], partner)

        self.start(group[0], None, r1.at[0], p1)
        self.start(group[0], None, r1.at[1], m1)
        second(0)
        tasks[0]()
        self.arrive(group[1], None, r1.at[0])
        self.start(group[1], 0, r1.at[2], p1)
        second(1)
        self.arrive(group[2], None, r1.at[1])
        self.start(group[2], 1, r1.at[3], m1)
        second(2)
        tasks[1]()
        relay(0)
        self.arrive(group[3], 0, r1.at[2])
        self.arrive(group[3], 1, r1.at[3])
        second(3)
        for q in (1, 2, 3):
            relay(q)
        for q in range(4):
            block = near(pos[q], 2)
            for i in range(2):
                self.arrive(block, i, r2.at[q, 2 + i])
            self.start(block, None, rp.at[12 + q], partner)
        for i in range(16):
            self.arrive(partner, None, rp.at[i])
        every = self.full.at[:, 0:31]
        pltpu.make_async_copy(every, every, self.ssem).wait()


def main_kernel(d, f_h, dg_h, w_h, pf_h, pi_h, perm_h, dft_h, df, full,
                perm, dft, wsum, f, dg, w, pf, pi, pw, pwt, pv, pvt, stage, stage2, spec, turn, spec2, send, recv, ship, shipr,
                isem, esem, gsem, r1, r2, rp):
    me = lax.axis_index("lat")
    tor = Torus(d, me)
    bar = pltpu.get_barrier_semaphore()
    loads = [pltpu.make_async_copy(f_h.at[c * d.bt:(c + 1) * d.bt], f.at[c * d.bt:(c + 1) * d.bt], isem.at[c]) for c in range(d.nc)]
    ah, al, bh, bl, sh, sl, zh, zl = [dft.at[i] for i in range(8)]
    tables = pltpu.make_async_copy(dft_h, dft, isem.at[d.nc + 7 + d.t])
    small = [pltpu.make_async_copy(perm_h, perm, isem.at[d.nc + 8 + d.t])]
    for k in range(d.t):
        small.append(pltpu.make_async_copy(pf_h.at[me + k * d.n], pf.at[k], isem.at[d.nc + 2 * k]))
        small.append(pltpu.make_async_copy(pi_h.at[me + k * d.n], pi.at[k], isem.at[d.nc + 2 * k + 1]))
    wloads = [pltpu.make_async_copy(w_h.at[j], full.at[j], isem.at[d.nc + 6 + j]) for j in range(d.t)]
    gload = pltpu.make_async_copy(dg_h, dg, isem.at[d.nc + 6 + d.t])
    for c in loads[:1] + [tables] + loads[1:]:
        c.start()

    def greet(k, _):
        pl.semaphore_signal(bar, inc=1, device_id={"lat": lax.rem(me + k, d.n)}, device_id_type=MESH)
        return 0
    lax.fori_loop(1, d.n, greet, 0)

    def exchange(e, snd, rcv):
        return Exchange(d, me, tor, snd, rcv, esem.at[e])

    ex = [[exchange(i * d.nc + c, send.at[i, c], recv.at[i, c])
           for c in range(d.nc)] for i in range(4)]
    ships = [[exchange((4 + i) * d.nc + c, ship.at[i, c], shipr.at[i, c]) for c in range(d.nc)] for i in range(2)]

    def pack(i, c, st):
        def fill(s):
            send[i, c, s] = st[message_rows(d, s), :].astype(BF16)
        loop(d.n, fill, 4)

    def dispatch(i, c, st):
        pack(i, c, st)
        ex[i][c].start()

    def collect(i, c, st):
        ex[i][c].collect()

        def take(s):
            st[message_rows(d, s), :] = recv[i, c, s].astype(F32)
        loop(d.n, take, 4)

    for c in range(d.nc):
        loads[c].wait()
        if c == 0:
            tables.wait()
            for x in small + wloads + [gload]:
                x.start()

        def analysis_step(p):
            bt = c * d.bt + 2 * p
            y = analyse(jnp.concatenate([f[bt], f[bt + 1]], axis=1), ah, al)
            for u, half in enumerate(lane_halves(d)):
                put_modes(d, stage, y, 2 * p + u, half)
        loop(d.bt // 2, analysis_step, 3)
        pack(0, c, stage)
    pl.semaphore_wait(bar, d.n - 1)
    for e in ex[0]:
        e.start()
    for x in small:
        x.wait()
    permuted(d, perm, pf, pw, pwt)
    permuted(d, perm, pi, pv, pvt)
    for j in range(d.t):
        wloads[j].wait()

        def prepare(ll):
            for r in range(2):
                w[d.n * j + ll, r * d.c:(r + 1) * d.c, :] = full[j, ll, pl.ds(r, d.c, stride=2), :].astype(BF16)
        loop(d.n, prepare, 4)

    for c in range(d.nc):
        collect(0, c, stage2)
        to_spectral(d, stage2, spec, turn, pw, 1.0)
        extract(d, spec, ship.at[0, c])
        mix(d, spec, turn, spec2, w, True)
        from_spectral(d, spec2, stage, pvt)
        dispatch(1, c, stage)
    for c in range(d.nc):
        ships[0][c].start()
    gload.wait()
    for c in range(d.nc):
        collect(1, c, stage2)

        def grid_step(p):
            bt = 2 * p
            at = c * d.bt + bt
            g = jnp.concatenate([get_modes(d, stage2, bt), get_modes(d, stage2, bt + 1)], axis=1).astype(BF16)
            h = mm(sh[...], g) + mm(sl[...], g)
            u = jnp.concatenate([dg[at], dg[at + 1]], axis=1) * gelu_grad(h)
            y = analyse(u, bh, bl)
            for i, half in enumerate(lane_halves(d)):
                put_modes(d, stage, y, bt + i, half)
        loop(d.bt // 2, grid_step, 2)
        dispatch(2, c, stage)
    for c in range(d.nc):
        collect(2, c, stage2)
        to_spectral(d, stage2, spec, turn, pv, -1.0)
        extract(d, spec, ship.at[1, c])
        ships[1][c].start()
        mix(d, spec, turn, spec2, w, False)
        from_spectral(d, spec2, stage, pwt)
        dispatch(3, c, stage)
        if c + 1 == d.nc:
            for e in ships[0] + ships[1][:c]:
                e.collect()
    for c in range(d.nc):
        if c + 1 == d.nc:
            ships[1][c].collect()
        for j, y in enumerate(weights(d, shipr.at[0, c], shipr.at[1, c])):
            if c + 1 < d.nc:
                wsum[j] = y if c == 0 else wsum[j] + y
            else:
                y = wsum[j] + y
                for r, half in enumerate(lane_halves(d)):
                    full[j, me, pl.ds(r, d.c, stride=2), :] = y[:, half]
    gather = Gather(d, me, tor, full, gsem.at[0], r1, r2, rp)

    def finish(c):
        def task():
            collect(3, c, stage2)

            def step(p):
                bt = 2 * p
                at = c * d.bt + bt
                g = jnp.concatenate([get_modes(d, stage2, bt), get_modes(d, stage2, bt + 1)], axis=1).astype(BF16)
                y = mm(zh[...], g) + mm(zl[...], g)
                for i, half in enumerate(lane_halves(d)):
                    df[at + i] = dg[at + i] + y[:, half]
            loop(d.bt // 2, step, 2)
        return task
    gather.run([finish(c) for c in range(d.nc)])
    for e in sum(ex + ships, []):
        e.drain()


def final_kernel(df, full, out, dw, sem):
    copies = [pltpu.make_async_copy(full.at[j], dw.at[j], sem.at[j]) for j in range(full.shape[0])]
    copies.append(pltpu.make_async_copy(df, out, sem.at[full.shape[0]]))
    for c in copies:
        c.start()
    for c in copies:
        c.wait()


def solution(mesh):
    n = mesh.shape['lat']
    field_spec = P('member', None, 'lat', None)

    def local_step(field_loc, grad_loc, p_fwd, p_inv, w_mix):
        batch, chan, rows, lon = field_loc.shape
        d = Dims(n, batch, chan, rows, lon)
        tables = np.stack([m for pair in dft_constants(d) for m in pair])
        perm = perm_constant(d)
        f = field_loc.transpose(0, 2, 3, 1).reshape(batch * rows, lon, chan)
        dg = grad_loc.transpose(0, 2, 3, 1).reshape(batch * rows, lon, chan)
        w = w_mix.transpose(0, 1, 3, 2).reshape(rows, n, 2 * chan, chan)

        nc = d.nc
        shipped = VMEM((2, nc, n, d.ship_off[-1], chan), BF16)
        message = VMEM((4, nc, n, d.msg, chan), BF16)
        stage = VMEM((n * d.msg, chan), F32)
        spec = VMEM((2 * rows * d.b * d.lp, chan), F32)
        mat = VMEM((rows, d.lat, d.lat), BF16)
        raw = VMEM((rows, d.lat, d.lat), F32)
        field = VMEM(f.shape, F32)
        dma = lambda *s: pltpu.SemaphoreType.DMA(s)
        vspec = pl.BlockSpec(memory_space=VMEM)
        hspec = pl.BlockSpec(memory_space=pltpu.HBM)
        df, full = pl.pallas_call(
            functools.partial(main_kernel, d), name="main",
            out_shape=[VMEM(f.shape, F32), VMEM(w.shape, F32)],
            in_specs=[hspec] * 7,
            out_specs=[vspec, vspec],
            scratch_shapes=[VMEM(perm.shape, BF16), VMEM(tables.shape, BF16), VMEM((rows, chan, 2 * chan), F32), field, field,
                            VMEM((d.lat, 2 * chan, chan), BF16), raw, raw, mat, mat, mat, mat, stage, stage, spec, spec, spec,
                            message, message, shipped, shipped,
                            dma(nc + 9 + rows), dma(6 * nc, 2), dma(1), dma(4), dma(4, 4), dma(16)],
            compiler_params=pltpu.CompilerParams(collective_id=0, has_side_effects=True, vmem_limit_bytes=49 * 1024 * 1024),
        )(f, dg, w, p_fwd, p_inv, perm, tables)
        df, dw = pl.pallas_call(
            final_kernel, name="final",
            out_shape=[jax.ShapeDtypeStruct(f.shape, F32), jax.ShapeDtypeStruct(w.shape, F32)],
            in_specs=[vspec, vspec], out_specs=[hspec, hspec],
            scratch_shapes=[dma(rows + 1)],
            compiler_params=pltpu.CompilerParams(vmem_limit_bytes=1024 * 1024),
        )(df, full)
        grad_field = df.reshape(batch, rows, lon, chan).transpose(0, 3, 1, 2)
        grad_wmix = dw.reshape(d.lat, chan, 2, chan).transpose(0, 1, 3, 2)
        return grad_field, grad_wmix

    return jax.shard_map(local_step, mesh=mesh, in_specs=(field_spec, field_spec, P(), P(), P()), out_specs=(field_spec, P('member', None, None, None)), check_vma=False)
```

```python
import functools
import math
import random
import numpy as np
import jax
import jax.numpy as jnp
from jax import lax
from jax.experimental import pallas as pl
from jax.experimental.pallas import tpu as pltpu
from jax.sharding import PartitionSpec as P

MESH = pl.DeviceIdType.MESH
F32, BF16 = jnp.float32, jnp.bfloat16
VMEM = pltpu.VMEM


class Dims:
    def __init__(self, n, batch, chan, rows, lon):
        self.n = n
        self.side = math.isqrt(n // 2)
        self.seed = 4
        self.nc = 2
        self.b, self.c, self.t, self.lon = batch // self.nc, chan, rows, lon
        self.lat = n * rows
        self.bt = self.b * rows
        self.msg = 2 * rows * self.bt
        self.lp = self.lat + 8
        self.ship_off = [self.b * j * (j + 1) for j in range(rows + 1)]


def split_const(mat):
    hi = mat.astype(jnp.bfloat16)
    lo = (mat - hi.astype(np.float64)).astype(jnp.bfloat16)
    return hi, lo


def dft_constants(d):
    m = np.arange(d.lat)
    ang = 2.0 * np.pi * np.outer(m, np.arange(d.lon)) / d.lon
    scale = 1.0 / math.sqrt(d.lon)
    ana = scale * np.concatenate([np.cos(ang), -np.sin(ang)])
    gain = np.where(m == 0, 1.0, 2.0)[:, None]
    ana2 = scale * np.concatenate([np.cos(ang) * gain, -np.sin(ang) * gain])
    syn = ana2.T
    syn2 = ana.T
    return [split_const(a) for a in (ana, ana2, syn, syn2)]


def perm_constant(d):
    t = np.arange(d.lat)
    tau = (t % d.t) * d.n + t // d.t
    mat = np.zeros((d.lat, d.lat))
    mat[t, tau] = 1.0
    return mat.astype(jnp.bfloat16)


def mm(a, b):
    return jnp.dot(a, b, preferred_element_type=F32)


def mm_nt(a, b):
    return lax.dot_general(a, b, (((1,), (1,)), ((), ())), preferred_element_type=F32)


def mm_tn(a, b):
    return lax.dot_general(a, b, (((0,), (0,)), ((), ())), preferred_element_type=F32)


def rnd(x):
    return x.astype(BF16).astype(F32)


class Torus:
    def __init__(self, d, me):
        side = d.side
        y, x, h = me // (2 * side), lax.rem(me // 2, side), lax.rem(me, 2)
        self.side, self.h = side, h
        way = 1 - 2 * h
        self.ys = [lax.rem(y + way * i + side, side) * (2 * side) for i in range(side)]
        self.xs = [lax.rem(x + way * i + side, side) * 2 for i in range(side)]
        self.hs = [h, 1 - h]

    def at(self, dy, dx, dh):
        return self.ys[dy % self.side] + self.xs[dx % self.side] + self.hs[dh % 2]


def remote(src, dst, ssem, rsem, to):
    return pltpu.make_async_remote_copy(src_ref=src, dst_ref=dst, send_sem=ssem, recv_sem=rsem,
                                        device_id={"lat": to}, device_id_type=MESH)


class Exchange:
    def __init__(self, d, me, tor, send, recv, sems):
        self.d, self.me, self.tor, self.send, self.recv = d, me, tor, send, recv
        self.ssem, self.rsem = sems.at[0], sems.at[1]
        self.offsets = [(dy, dx, dh) for dy in range(d.side) for dx in range(d.side) for dh in range(2)][1:]
        random.Random(d.seed).shuffle(self.offsets)

    def start(self):
        for o in self.offsets:
            to = self.tor.at(*o)
            remote(self.send.at[to], self.recv.at[self.me], self.ssem, self.rsem, to).start()

    def wait(self, ref, sem):
        pltpu.make_async_copy(ref, ref, sem).wait()

    def collect(self):
        self.recv[self.me] = self.send[self.me]
        self.wait(self.recv.at[0:self.d.n - 1], self.rsem)

    def drain(self):
        self.wait(self.send.at[0:self.d.n - 1], self.ssem)


def message_rows(d, s):
    return pl.ds(pl.multiple_of(s * d.msg, 8), d.msg)


def ring_rows(d, start):
    return pl.ds(start, d.n, stride=d.msg)


def put_modes(d, stage, y, bt, lanes):
    for rk in range(2 * d.t):
        stage[ring_rows(d, rk * d.bt + bt), :] = y[rk * d.n:(rk + 1) * d.n, lanes]


def get_modes(d, stage, bt):
    return jnp.concatenate([stage[ring_rows(d, rk * d.bt + bt), :] for rk in range(2 * d.t)], axis=0)


def analyse(x, hi, lo):
    xh = x.astype(BF16)
    xl = (x - xh.astype(F32)).astype(BF16)
    return mm(hi[...], xh) + mm(lo[...], xh) + mm(hi[...], xl)


def loop(count, body, unroll=1):
    def step(i, _):
        body(i)
        return 0
    lax.fori_loop(0, count, step, 0, unroll=unroll)


def lane_halves(d):
    return slice(0, d.c), slice(d.c, 2 * d.c)


def permuted(d, perm, p, out, outt):
    for k in range(d.t):
        pk = p[k].astype(BF16)
        out[k] = mm(pk, perm[...]).astype(BF16)
        outt[k] = mm_tn(perm[...], pk.T).astype(BF16)


def spec_at(d, r, k, b):
    return pl.multiple_of(((k * 2 + r) * d.b + b) * d.lp + d.n * k, 8)


def to_spectral(d, stage, spec, turn, p, sign):
    for k in range(d.t):
        low = d.n * k

        def body(b):
            x = jnp.concatenate([jnp.concatenate(
                [stage[ring_rows(d, (r * d.t + k) * d.bt + b * d.t + t), :] for t in range(d.t)], axis=0)
                for r in range(2)], axis=1)
            y = rnd(mm(p[k, low:, :], x.astype(BF16)))
            for r, half in enumerate(lane_halves(d)):
                spec[pl.ds(spec_at(d, r, k, b), d.lat - low), :] = y[:, half]
                turn[pl.ds(spec_at(d, 1 - r, k, b), d.lat - low), :] = y[:, half] * (sign if r == 0 else -sign)
        loop(d.b, body, d.b)


def from_spectral(d, spec, stage, pt):
    for k in range(d.t):
        low = d.n * k

        def body(b):
            x = jnp.concatenate([spec[pl.ds(spec_at(d, r, k, b), d.lat - low), :] for r in range(2)], axis=1).astype(BF16)
            y = mm(pt[k][:, low:], x)
            for r, half in enumerate(lane_halves(d)):
                for t in range(d.t):
                    stage[ring_rows(d, (r * d.t + k) * d.bt + b * d.t + t), :] = y[t * d.n:(t + 1) * d.n, half]
        loop(d.b, body, d.b)


def extract(d, spec, ship):
    for j in range(d.t):
        def body(ll):
            ship[ll, d.ship_off[j]:d.ship_off[j + 1], :] = spec[pl.ds(d.n * j + ll, 2 * d.b * (j + 1), stride=d.lp), :].astype(BF16)
        loop(d.n, body, 8)


def mix(d, spec, turn, out, w, forward):
    for j in range(d.t):
        rows = 2 * d.b * (j + 1)

        def body(ll):
            l = d.n * j + ll
            at = pl.ds(l, rows, stride=d.lp)
            x = spec[at, :].astype(BF16)
            x2 = jnp.concatenate([x, turn[at, :].astype(BF16)], axis=1)
            if forward:
                y = mm_nt(x2, jnp.concatenate([w[l, :d.c, :], w[l, d.c:, :]], axis=1))
            else:
                y = mm(x2, w[l])
            out[at, :] = rnd(y)
        loop(d.n, body, 8)


def gelu_grad(values):
    cumulative = 0.5 * (1.0 + lax.erf(values * math.sqrt(0.5)))
    density = jnp.exp(-0.5 * values * values) * (1.0 / math.sqrt(2.0 * math.pi))
    return cumulative + values * density


def weights(d, a, dq):
    parts = []
    for j in range(d.t):
        at = slice(d.ship_off[j], d.ship_off[j + 1])
        groups = d.n * (j + 1)
        x = a[:, at, :].astype(F32).reshape(groups, 2 * d.b, d.c)
        turn = jnp.concatenate([-x[:, d.b:, :], x[:, :d.b, :]], axis=1)
        both = jnp.concatenate([x, turn], axis=2).reshape(groups * 2 * d.b, 2 * d.c)
        g = dq[:, at, :].astype(F32).reshape(groups * 2 * d.b, d.c)
        parts.append(mm_tn(g.astype(BF16), both.astype(BF16)))
    return parts


class Gather:
    def __init__(self, d, me, tor, full, ssem, r1, r2, rp):
        self.d, self.me, self.tor, self.full = d, me, tor, full
        self.ssem, self.r1, self.r2, self.rp = ssem, r1, r2, rp
        self.half = full.shape[2] // 2
        h, side = tor.h, tor.side
        self.first = [lax.select(h == 0, tor.xs[i], tor.ys[i]) for i in range(side)]
        self.second = [lax.select(h == 0, tor.ys[i], tor.xs[i]) for i in range(side)]

    def near(self, one, two):
        return self.first[one % self.d.side] + self.second[two % self.d.side] + self.tor.h

    def piece(self, block, part):
        if part is None:
            return self.full.at[:, block]
        return self.full.at[:, block, self.half * part:self.half * (part + 1), :]

    def start(self, block, part, rsem, to):
        ref = self.piece(block, part)
        remote(ref, ref, self.ssem, rsem, to).start()

    def arrive(self, block, part, rsem):
        ref = self.piece(block, part)
        pltpu.make_async_copy(ref, ref, rsem).wait()

    def run(self, tasks):
        near, r1, r2, rp = self.near, self.r1, self.r2, self.rp
        partner = self.tor.at(0, 0, 1)
        pos = [0, -1, 1, 2]
        p1, m1, p2, m2 = near(1, 0), near(-1, 0), near(0, 1), near(0, -1)
        group = [near(i, 0) for i in pos]

        def second(q):
            self.start(group[q], None, r2.at[q, 0], p2)
            self.start(group[q], None, r2.at[q, 1], m2)
            self.start(group[q], None, rp.at[q], partner)

        def relay(q):
            for i, (off, to) in enumerate(((-1, p2), (1, m2))):
                block = near(pos[q], off)
                self.arrive(block, None, r2.at[q, i])
                self.start(block, i, r2.at[q, 2 + i], to)
                self.start(block, None, rp.at[4 + 2 * q + i], partner)

        self.start(group[0], None, r1.at[0], p1)
        self.start(group[0], None, r1.at[1], m1)
        second(0)
        tasks[0]()
        self.arrive(group[1], None, r1.at[0])
        self.start(group[1], 0, r1.at[2], p1)
        second(1)
        self.arrive(group[2], None, r1.at[1])
        self.start(group[2], 1, r1.at[3], m1)
        second(2)
        relay(0)
        self.arrive(group[3], 0, r1.at[2])
        self.arrive(group[3], 1, r1.at[3])
        second(3)
        tasks[1]()
        for q in (1, 2, 3):
            relay(q)
        for q in range(4):
            block = near(pos[q], 2)
            for i in range(2):
                self.arrive(block, i, r2.at[q, 2 + i])
            self.start(block, None, rp.at[12 + q], partner)
        for i in range(16):
            self.arrive(partner, None, rp.at[i])
        every = self.full.at[:, 0:31]
        pltpu.make_async_copy(every, every, self.ssem).wait()


def main_kernel(d, f_h, dg_h, w_h, pf_h, pi_h, perm_h, dft_h, df, full,
                perm, dft, wsum, f, dg, w, pf, pi, pw, pwt, pv, pvt, stage, stage2, spec, turn, spec2, send, recv, ship, shipr,
                isem, esem, gsem, r1, r2, rp):
    me = lax.axis_index("lat")
    tor = Torus(d, me)
    bar = pltpu.get_barrier_semaphore()
    loads = [pltpu.make_async_copy(f_h.at[c * d.bt:(c + 1) * d.bt], f.at[c * d.bt:(c + 1) * d.bt], isem.at[c]) for c in range(d.nc)]
    ah, al, bh, bl, sh, sl, zh, zl = [dft.at[i] for i in range(8)]
    tables = pltpu.make_async_copy(dft_h, dft, isem.at[d.nc + 7 + d.t])
    small = [pltpu.make_async_copy(perm_h, perm, isem.at[d.nc + 8 + d.t])]
    for k in range(d.t):
        small.append(pltpu.make_async_copy(pf_h.at[me + k * d.n], pf.at[k], isem.at[d.nc + 2 * k]))
        small.append(pltpu.make_async_copy(pi_h.at[me + k * d.n], pi.at[k], isem.at[d.nc + 2 * k + 1]))
    wloads = [pltpu.make_async_copy(w_h.at[j], full.at[j], isem.at[d.nc + 6 + j]) for j in range(d.t)]
    gload = pltpu.make_async_copy(dg_h, dg, isem.at[d.nc + 6 + d.t])
    for c in loads[:1] + [tables] + loads[1:]:
        c.start()

    def greet(k, _):
        pl.semaphore_signal(bar, inc=1, device_id={"lat": lax.rem(me + k, d.n)}, device_id_type=MESH)
        return 0
    lax.fori_loop(1, d.n, greet, 0)

    def exchange(e, snd, rcv):
        return Exchange(d, me, tor, snd, rcv, esem.at[e])

    ex = [[exchange(i * d.nc + c, send.at[i, c], recv.at[i, c])
           for c in range(d.nc)] for i in range(4)]
    ships = [[exchange((4 + i) * d.nc + c, ship.at[i, c], shipr.at[i, c]) for c in range(d.nc)] for i in range(2)]

    def pack(i, c, st):
        def fill(s):
            send[i, c, s] = st[message_rows(d, s), :].astype(BF16)
        loop(d.n, fill, 4)

    def dispatch(i, c, st):
        pack(i, c, st)
        ex[i][c].start()

    def collect(i, c, st):
        ex[i][c].collect()

        def take(s):
            st[message_rows(d, s), :] = recv[i, c, s].astype(F32)
        loop(d.n, take, 4)

    for c in range(d.nc):
        loads[c].wait()
        if c == 0:
            tables.wait()
            for x in small + wloads + [gload]:
                x.start()

        def analysis_step(p):
            bt = c * d.bt + 2 * p
            y = analyse(jnp.concatenate([f[bt], f[bt + 1]], axis=1), ah, al)
            for u, half in enumerate(lane_halves(d)):
                put_modes(d, stage, y, 2 * p + u, half)
        loop(d.bt // 2, analysis_step, 3)
        pack(0, c, stage)
    pl.semaphore_wait(bar, d.n - 1)
    for e in ex[0]:
        e.start()
    for x in small:
        x.wait()
    permuted(d, perm, pf, pw, pwt)
    permuted(d, perm, pi, pv, pvt)
    for j in range(d.t):
        wloads[j].wait()

        def prepare(ll):
            for r in range(2):
                w[d.n * j + ll, r * d.c:(r + 1) * d.c, :] = full[j, ll, pl.ds(r, d.c, stride=2), :].astype(BF16)
        loop(d.n, prepare, 4)

    for c in range(d.nc):
        collect(0, c, stage2)
        to_spectral(d, stage2, spec, turn, pw, 1.0)
        extract(d, spec, ship.at[0, c])
        mix(d, spec, turn, spec2, w, True)
        from_spectral(d, spec2, stage, pvt)
        dispatch(1, c, stage)
    for c in range(d.nc):
        ships[0][c].start()
    gload.wait()
    for c in range(d.nc):
        collect(1, c, stage2)

        def grid_step(p):
            bt = 2 * p
            at = c * d.bt + bt
            g = jnp.concatenate([get_modes(d, stage2, bt), get_modes(d, stage2, bt + 1)], axis=1).astype(BF16)
            h = mm(sh[...], g) + mm(sl[...], g)
            u = jnp.concatenate([dg[at], dg[at + 1]], axis=1) * gelu_grad(h)
            y = analyse(u, bh, bl)
            for i, half in enumerate(lane_halves(d)):
                put_modes(d, stage, y, bt + i, half)
        loop(d.bt // 2, grid_step, 2)
        dispatch(2, c, stage)
    for c in range(d.nc):
        collect(2, c, stage2)
        to_spectral(d, stage2, spec, turn, pv, -1.0)
        extract(d, spec, ship.at[1, c])
        ships[1][c].start()
        mix(d, spec, turn, spec2, w, False)
        from_spectral(d, spec2, stage, pwt)
        dispatch(3, c, stage)
        if c + 1 == d.nc:
            for e in ships[0] + ships[1][:c]:
                e.collect()
    for c in range(d.nc):
        if c + 1 == d.nc:
            ships[1][c].collect()
        for j, y in enumerate(weights(d, shipr.at[0, c], shipr.at[1, c])):
            if c + 1 < d.nc:
                wsum[j] = y if c == 0 else wsum[j] + y
            else:
                y = wsum[j] + y
                for r, half in enumerate(lane_halves(d)):
                    full[j, me, pl.ds(r, d.c, stride=2), :] = y[:, half]
    gather = Gather(d, me, tor, full, gsem.at[0], r1, r2, rp)

    def finish(c):
        def task():
            collect(3, c, stage2)

            def step(p):
                bt = 2 * p
                at = c * d.bt + bt
                g = jnp.concatenate([get_modes(d, stage2, bt), get_modes(d, stage2, bt + 1)], axis=1).astype(BF16)
                y = mm(zh[...], g) + mm(zl[...], g)
                for i, half in enumerate(lane_halves(d)):
                    df[at + i] = dg[at + i] + y[:, half]
            loop(d.bt // 2, step, 2)
        return task
    gather.run([finish(c) for c in range(d.nc)])
    for e in sum(ex + ships, []):
        e.drain()


def final_kernel(df, full, out, dw, sem):
    copies = [pltpu.make_async_copy(full.at[j], dw.at[j], sem.at[j]) for j in range(full.shape[0])]
    copies.append(pltpu.make_async_copy(df, out, sem.at[full.shape[0]]))
    for c in copies:
        c.start()
    for c in copies:
        c.wait()


def solution(mesh):
    n = mesh.shape['lat']
    field_spec = P('member', None, 'lat', None)

    def local_step(field_loc, grad_loc, p_fwd, p_inv, w_mix):
        batch, chan, rows, lon = field_loc.shape
        d = Dims(n, batch, chan, rows, lon)
        tables = np.stack([m for pair in dft_constants(d) for m in pair])
        perm = perm_constant(d)
        f = field_loc.transpose(0, 2, 3, 1).reshape(batch * rows, lon, chan)
        dg = grad_loc.transpose(0, 2, 3, 1).reshape(batch * rows, lon, chan)
        w = w_mix.transpose(0, 1, 3, 2).reshape(rows, n, 2 * chan, chan)

        nc = d.nc
        shipped = VMEM((2, nc, n, d.ship_off[-1], chan), BF16)
        message = VMEM((4, nc, n, d.msg, chan), BF16)
        stage = VMEM((n * d.msg, chan), F32)
        spec = VMEM((2 * rows * d.b * d.lp, chan), F32)
        mat = VMEM((rows, d.lat, d.lat), BF16)
        raw = VMEM((rows, d.lat, d.lat), F32)
        field = VMEM(f.shape, F32)
        dma = lambda *s: pltpu.SemaphoreType.DMA(s)
        vspec = pl.BlockSpec(memory_space=VMEM)
        hspec = pl.BlockSpec(memory_space=pltpu.HBM)
        df, full = pl.pallas_call(
            functools.partial(main_kernel, d), name="main",
            out_shape=[VMEM(f.shape, F32), VMEM(w.shape, F32)],
            in_specs=[hspec] * 7,
            out_specs=[vspec, vspec],
            scratch_shapes=[VMEM(perm.shape, BF16), VMEM(tables.shape, BF16), VMEM((rows, chan, 2 * chan), F32), field, field,
                            VMEM((d.lat, 2 * chan, chan), BF16), raw, raw, mat, mat, mat, mat, stage, stage, spec, spec, spec,
                            message, message, shipped, shipped,
                            dma(nc + 9 + rows), dma(6 * nc, 2), dma(1), dma(4), dma(4, 4), dma(16)],
            compiler_params=pltpu.CompilerParams(collective_id=0, has_side_effects=True, vmem_limit_bytes=49 * 1024 * 1024),
        )(f, dg, w, p_fwd, p_inv, perm, tables)
        df, dw = pl.pallas_call(
            final_kernel, name="final",
            out_shape=[jax.ShapeDtypeStruct(f.shape, F32), jax.ShapeDtypeStruct(w.shape, F32)],
            in_specs=[vspec, vspec], out_specs=[hspec, hspec],
            scratch_shapes=[dma(rows + 1)],
            compiler_params=pltpu.CompilerParams(vmem_limit_bytes=1024 * 1024),
        )(df, full)
        grad_field = df.reshape(batch, rows, lon, chan).transpose(0, 3, 1, 2)
        grad_wmix = dw.reshape(d.lat, chan, 2, chan).transpose(0, 1, 3, 2)
        return grad_field, grad_wmix

    return jax.shard_map(local_step, mesh=mesh, in_specs=(field_spec, field_spec, P(), P(), P()), out_specs=(field_spec, P('member', None, None, None)), check_vma=False)
```
